32 devices in a mesh: gx: 2 (over x), gy: 4 (over z), gz: 4 (over y, core).
Axes of the slice: x: 2, y: 2, z: 4, core: 2. Of those that a mesh axis runs over, the one named last changes fastest.
Arguments:
- calcium: float32 [8, 64, 128, 512], P(None, 'gx', 'gz', 'gy'), may hold values from 0.1 to 3
- activation: float32 [8, 64, 128, 512], P(None, 'gx', 'gz', 'gy'), may hold values from 0 to 1
- element_first: int32 [64], replicated, may hold values from 0 to 15, as said below
- offset_first: float32 [64], replicated, may hold values from 0.1 to 0.9
- element_second: int32 [512], replicated, may hold values from 0 to 127, as said below
- offset_second: float32 [512], replicated, may hold values from 0.1 to 0.9
- element_third: int32 [128], replicated, may hold values from 0 to 31, as said below
- offset_third: float32 [128], replicated, may hold values from 0.1 to 0.9
- troponin: float32 [16, 32, 128], P('gx', ('gy', 'gz')), may hold values from 0 to 1
- tension: float32 [16, 32, 128], P('gx', ('gy', 'gz')), may hold values from 0 to 2
- unbind_rate: float32 [16, 32, 128], P('gx', ('gy', 'gz')), may hold values from 0.2 to 2
- relax_rate: float32 [16, 32, 128], P('gx', ('gy', 'gz')), may hold values from 0.5 to 4
Outputs:
- bound_fraction: float32 [16, 32, 128], P('gx', ('gy', 'gz'))
- active_tension: float32 [16, 32, 128], P('gx', ('gy', 'gz'))
The draws below stay inside these ranges and needn't reach their ends.
Inputs may be any that keep to these rules, and one draw needn't show every extreme that they name: `element_first`: never falling; the cells of each aligned block of 32 cells belong to that block's own 8 elements, each element holding at least one cell. `element_second`: never falling; the cells of each aligned block of 128 cells belong to that block's own 32 elements, each element holding at least one cell. `element_third`: never falling; the cells of each aligned block of 8 cells belong to that block's own 2 elements, each element holding at least one cell.
All inputs are finite; a program needn't handle non-finite values.
Results may differ from the reference program's by a relative error of at most 0.00005.
Values sent between devices are 32-bit elements.
A program may use at most 64 MiB of HBM per device.

```python
import math
import jax
import jax.numpy as jnp
from jax import lax

EX_DEV = 8
EY_DEV = 32
EZ_BLK = 2
SUB = 8
FX_BLK = 32
FY_BLK = 128
FZ_BLK = 8
NXC = 16
NYC = 128
NZC = 32
NXF = 64
NYF = 512
NZF = 128


def block_elements(key, blocks, cells, elements):

    def single(block_key):
        scores = jax.random.permutation(block_key, cells - 1) + 1
        cut_points = jnp.sort(scores[:elements - 1])
        places = jnp.arange(cells)
        return jnp.sum((places[:, None] >= cut_points[None, :]).astype(jnp.int32), axis=1)
    block_keys = jax.random.split(key, blocks)
    within = jax.vmap(single)(block_keys)
    offsets = elements * jnp.arange(blocks)[:, None]
    return (within + offsets).reshape(-1).astype(jnp.int32)


def draw_element_first(key, part):
    return block_elements(jax.random.fold_in(key, 11), NXF // FX_BLK, FX_BLK, EX_DEV)


def draw_element_second(key, part):
    return block_elements(jax.random.fold_in(key, 23), NYF // FY_BLK, FY_BLK, EY_DEV)


def draw_element_third(key, part):
    return block_elements(jax.random.fold_in(key, 37), NZF // FZ_BLK, FZ_BLK, EZ_BLK)


def block_scale(rng, extent, cuts, least, largest):
    level, own = 1.0, jax.random.fold_in(rng, 6)
    for dim, shards_of in cuts:
        draws = jnp.exp(jax.random.uniform(jax.random.fold_in(own, dim), (shards_of,), jnp.float32, least / len(cuts), largest / len(cuts)))
        level = level * jnp.repeat(draws, extent[dim] // shards_of).reshape([-1 if axis == dim else 1 for axis in range(len(extent))])
    return level


def setup_inputs(seed: int = 0) -> dict:
    streams_of = jax.random.split(jax.random.key(seed), 13)
    return {
        "calcium": jnp.clip(jnp.exp(math.log(3.0) - 3.4011974 * jax.random.uniform(streams_of[0], (SUB, NXF, NZF, NYF), jnp.float32) ** block_scale(streams_of[0], (SUB, NXF, NZF, NYF), ((1, 2), (2, 4), (3, 4)), -0.2, 0.2)), 0.1, 3.0),
        "activation": jnp.clip(1.0 * jax.random.uniform(streams_of[1], (SUB, NXF, NZF, NYF), jnp.float32) ** block_scale(streams_of[1], (SUB, NXF, NZF, NYF), ((1, 2), (2, 4), (3, 4)), -0.2, 0.2), 0.0, 1.0),
        "element_first": draw_element_first(jax.random.fold_in(streams_of[12], 71), 0),
        "offset_first": jnp.clip(jax.random.uniform(streams_of[3], (NXF,), jnp.float32, 0.1, 0.9), 0.1, 0.9),
        "element_second": draw_element_second(jax.random.fold_in(streams_of[12], 71), 0),
        "offset_second": jnp.clip(jax.random.uniform(streams_of[5], (NYF,), jnp.float32, 0.1, 0.9), 0.1, 0.9),
        "element_third": draw_element_third(jax.random.fold_in(streams_of[12], 71), 0),
        "offset_third": jnp.clip(jax.random.uniform(streams_of[7], (NZF,), jnp.float32, 0.1, 0.9), 0.1, 0.9),
        "troponin": jnp.clip(1.0 * jax.random.uniform(streams_of[8], (NXC, NZC, NYC), jnp.float32) ** block_scale(streams_of[8], (NXC, NZC, NYC), ((0, 2), (1, 16)), -0.2, 0.2), 0.0, 1.0),
        "tension": jnp.clip(2.0 * jax.random.uniform(streams_of[9], (NXC, NZC, NYC), jnp.float32) ** block_scale(streams_of[9], (NXC, NZC, NYC), ((0, 2), (1, 16)), -0.2, 0.2), 0.0, 2.0),
        "unbind_rate": jnp.clip(jnp.exp(math.log(2.0) - 2.3025851 * jax.random.uniform(streams_of[10], (NXC, NZC, NYC), jnp.float32) ** block_scale(streams_of[10], (NXC, NZC, NYC), ((0, 2), (1, 16)), -0.2, 0.2)), 0.2, 2.0),
        "relax_rate": jnp.clip(jnp.exp(math.log(4.0) - 2.0794415 * jax.random.uniform(streams_of[11], (NXC, NZC, NYC), jnp.float32) ** block_scale(streams_of[11], (NXC, NZC, NYC), ((0, 2), (1, 16)), -0.2, 0.2)), 0.5, 4.0),
    }


highest = lax.Precision.HIGHEST
step_size = 0.2
bind_rate = 2.0
peak_tension = 2.0
half_square = 0.25


def weights(element, offset, count):
    node_ids = jnp.arange(count, dtype=jnp.int32)
    inside = element[None, :] == node_ids[:, None]
    following = element[None, :] + 1 == node_ids[:, None]
    raw_weights = jnp.where(inside, 1.0 - offset[None, :], 0.0) + jnp.where(following, offset[None, :], 0.0)
    return raw_weights / jnp.sum(raw_weights, axis=1, keepdims=True)


def restrict(field, weight_row, weight_depth, weight_col):
    section = jnp.einsum("ai,izy->azy", weight_row, field, precision=highest)
    section = jnp.einsum("bz,azy->aby", weight_depth, section, precision=highest)
    return jnp.einsum("cy,aby->abc", weight_col, section, precision=highest)


def reference(calcium, activation, element_first, offset_first, element_second, offset_second, element_third, offset_third, troponin, tension, unbind_rate, relax_rate):
    weight_row = weights(element_first, offset_first, NXC)
    weight_col = weights(element_second, offset_second, NYC)
    weight_depth = weights(element_third, offset_third, NZC)

    def single(index):
        return (restrict(calcium[index], weight_row, weight_depth, weight_col),
                restrict(activation[index], weight_row, weight_depth, weight_col))

    drive_calcium, drive_activation = lax.map(single, jnp.arange(SUB, dtype=jnp.int32))
    bound = troponin
    active = tension
    for substep in range(SUB):
        calcium_now = drive_calcium[substep]
        squared = calcium_now * calcium_now
        binding = squared / (squared + half_square)
        bound = bound + step_size * (bind_rate * binding * (1.0 - bound) - unbind_rate * bound)
        active = active + step_size * relax_rate * (peak_tension * drive_activation[substep] * bound - active)
    return bound, active
```

```python
import functools

import jax
import jax.numpy as jnp
from jax import lax
from jax.experimental import pallas as pl
from jax.experimental.pallas import tpu as pltpu
from jax.sharding import PartitionSpec as P

step_size = 0.2
bind_rate = 2.0
peak_tension = 2.0
half_square = 0.25
f32 = jnp.float32
bf16 = jnp.bfloat16
MESH = pl.DeviceIdType.MESH
CHUNKS = 2


def split(x):
    high = x.astype(bf16)
    return high, (x - high.astype(f32)).astype(bf16)


def node_weights(element, offset, node):
    raw = jnp.where(element == node, 1.0 - offset, 0.0) + jnp.where(
        element + 1 == node, offset, 0.0
    )
    total = jnp.sum(raw, axis=1, keepdims=True)
    return raw, jnp.where(total > 0.0, total, 1.0)


def expand(weight, pick):
    high, low = split(weight)
    return jnp.dot(high, pick, preferred_element_type=f32) + jnp.dot(
        low, pick, preferred_element_type=f32
    )


def iota(shape, dim):
    return lax.broadcasted_iota(jnp.int32, shape, dim)


def kernel(
    calcium,
    activation,
    *refs,
    sizes,
):
    small = refs[:10]
    out_bound, out_active, xc, xa = refs[10:14]
    local = refs[14:24]
    (
        main,
        third,
        edge,
        got_main,
        got_third,
        got_first,
        got_corner,
        load_sem,
        small_sem,
        send_main,
        send_edge,
        recv_main,
        recv_third,
        recv_first,
        recv_corner,
    ) = refs[24:]
    e1, o1, e2, o2, e3, o3, troponin, tension, unbind, relax = local
    nx, ny, nz = sizes
    subs, rows, depth, cols = xc.shape
    nodes_x, per_block, all_y = troponin.shape
    nodes_y = all_y // ny
    blocks = nz
    slab = per_block * blocks
    gx, gy, gz = lax.axis_index("gx"), lax.axis_index("gy"), lax.axis_index("gz")
    chunk = subs // CHUNKS

    def load(t):
        return (
            pltpu.make_async_copy(calcium.at[t], xc.at[t], load_sem.at[0, t]),
            pltpu.make_async_copy(activation.at[t], xa.at[t], load_sem.at[1, t]),
        )

    fetches = [
        pltpu.make_async_copy(source, target, small_sem.at[i])
        for i, (source, target) in enumerate(zip(small, local))
    ]
    for copy in fetches:
        copy.start()
    for t in range(subs):
        for copy in load(t):
            copy.start(priority=1)

    barrier = pltpu.get_barrier_semaphore()
    has_next_x = gx + 1 < nx
    has_next_z = gz + 1 < nz
    own = gy == gz
    from_third = jnp.logical_and(gz == 0, gy > 0)
    from_first = gx > 0
    from_corner = jnp.logical_and(from_third, from_first)
    for s in range(ny):

        def greet(dx, dz, s=s):
            pl.semaphore_signal(
                barrier, inc=1, device_id=(gx - dx, s, gy - dz), device_id_type=MESH
            )

        @pl.when(jnp.logical_not(jnp.logical_and(s == gy, own)))
        def _():
            greet(0, 0)

        @pl.when(jnp.logical_and(from_third, jnp.logical_not(jnp.logical_and(s == gy, gy - 1 == gz))))
        def _():
            greet(0, 1)

        @pl.when(from_first)
        def _():
            greet(1, 0)

        @pl.when(from_corner)
        def _():
            greet(1, 1)

    for copy in fetches[:6]:
        copy.wait()
    row_count = (slab + 1) * nodes_x + 16
    r = iota((row_count, 1), 0)
    inner = r < (slab + 1) * nodes_x
    tail = r - (slab + 1) * nodes_x
    node_a = jnp.where(inner, r % nodes_x, nodes_x)
    node_b = jnp.where(inner, r // nodes_x, per_block * (tail % 8) + tail // 8)
    raw, total = node_weights(e1[...], o1[...], node_a + gx * nodes_x)
    wide = rows * depth
    pick = (
        iota((raw.shape[1], wide), 0) == gx * rows + iota((raw.shape[1], wide), 1) // depth
    ).astype(bf16)
    weight_x = expand(raw / total, pick)
    raw, total = node_weights(e3[...], o3[...], node_b + gz * slab)
    pick = (
        iota((raw.shape[1], wide), 0) == gz * depth + iota((raw.shape[1], wide), 1) % depth
    ).astype(bf16)
    weight_z = expand(raw / total, pick)
    k_high, k_low = split(weight_x * weight_z)
    k_both = jnp.concatenate([k_high, k_low], axis=0)

    lanes = 2 * per_block * nodes_y
    n = iota((lanes, 1), 0)
    mine = pl.ds(pl.multiple_of(gy * cols, cols), cols)
    spread = []
    for ghost in range(2):
        node = gy * nodes_y + (nodes_y if ghost else n % nodes_y)
        node = node + jnp.zeros_like(n)
        total = node_weights(e2[...], o2[...], node)[1]
        weight = node_weights(e2[:, mine], o2[:, mine], node)[0] / total
        if ghost:
            weight = jnp.where(n % nodes_y == 0, weight, 0.0)
        spread.append(
            jnp.concatenate(
                [
                    jnp.where(n // nodes_y == f * per_block + b, weight, 0.0)
                    for b in range(per_block)
                    for f in range(2)
                ],
                axis=1,
            )
        )
    y_high, y_low = split(jnp.concatenate(spread, axis=0))

    def to_message(values):
        high, low = split(values)
        dims = (((1,), (1,)), ((), ()))
        dot = functools.partial(
            lax.dot_general, dimension_numbers=dims, preferred_element_type=f32
        )
        return dot(high, y_high) + dot(low, y_high) + dot(high, y_low)

    def part(c):
        first = c * chunk * nodes_x
        last = (c + 1) * chunk * nodes_x + (nodes_x if c == CHUNKS - 1 else 0)
        return pl.ds(first, last - first)

    def main_copy(q, c):
        return pltpu.make_async_remote_copy(
            src_ref=main.at[q, part(c)],
            dst_ref=got_main.at[gy, part(c)],
            send_sem=send_main.at[q, c],
            recv_sem=recv_main.at[gy, c],
            device_id=(gx, gz, q),
            device_id_type=MESH,
        )

    def third_part(c):
        step = chunk // per_block * nodes_x
        return pl.ds(c * step, step + (nodes_x if c == CHUNKS - 1 else 0))

    def third_copy(c):
        return pltpu.make_async_remote_copy(
            src_ref=third.at[third_part(c)],
            dst_ref=got_third.at[gy, third_part(c)],
            send_sem=send_main.at[blocks, c],
            recv_sem=recv_third.at[gy, c],
            device_id=(gx, gz + 1, 0),
            device_id_type=MESH,
        )

    def first_copy(q):
        return pltpu.make_async_remote_copy(
            src_ref=edge.at[q],
            dst_ref=got_first.at[gy],
            send_sem=send_edge.at[q],
            recv_sem=recv_first.at[gy],
            device_id=(gx + 1, gz, q),
            device_id_type=MESH,
        )

    def corner_copy():
        return pltpu.make_async_remote_copy(
            src_ref=edge.at[blocks],
            dst_ref=got_corner.at[gy],
            send_sem=send_edge.at[blocks],
            recv_sem=recv_corner.at[gy],
            device_id=(gx + 1, gz + 1, 0),
            device_id_type=MESH,
        )

    third_here = jnp.logical_and(gz == 0, gy == 1)
    third_away = jnp.logical_and(has_next_z, jnp.logical_not(third_here))

    def each_main(c, do):
        for q in range(blocks):

            @pl.when(jnp.logical_not(jnp.logical_and(own, gz == q)))
            def _(q=q):
                do(main_copy(q, c))

        @pl.when(third_away)
        def _():
            do(third_copy(c))

    def each_edge(do):
        @pl.when(has_next_x)
        def _():
            for q in range(blocks):
                do(first_copy(q))

        @pl.when(jnp.logical_and(has_next_x, has_next_z))
        def _():
            do(corner_copy())

    packed = pair = None
    tile = nodes_x
    for c in range(CHUNKS):
        gathered = []
        for t in range(c * chunk, (c + 1) * chunk):
            for copy in load(t):
                copy.wait()
            field = jnp.concatenate(
                [xc[t].reshape(wide, cols), xa[t].reshape(wide, cols)], axis=1
            )
            high, low = split(field)
            both = jnp.dot(k_both, high, preferred_element_type=f32)
            node = (
                both[:row_count]
                + both[row_count:]
                + jnp.dot(k_high, low, preferred_element_type=f32)
            )
            sides = []
            for k in range(per_block):
                pieces = []
                for q in range(blocks + 1):
                    b = q * per_block + k
                    if b <= slab:
                        pieces.append(node[b * tile : (b + 1) * tile])
                    else:
                        pieces.append(jnp.zeros((tile, 2 * cols), f32))
                base = (slab + 1) * tile + 8 * k
                pieces.append(node[base : base + 8])
                sides.append(jnp.concatenate(pieces, axis=0))
            gathered.append(jnp.concatenate(sides, axis=1))
        result = to_message(jnp.concatenate(gathered, axis=0))
        per = (blocks + 1) * tile + 8
        for k, t in enumerate(range(c * chunk, (c + 1) * chunk)):
            values = result[k * per : (k + 1) * per]
            for q in range(blocks):
                main[q, t * tile : (t + 1) * tile] = values[q * tile : (q + 1) * tile, :lanes]
            for q in range(blocks + 1):
                row = (blocks + 1) * tile + q
                edge[q, t : t + 1] = values[row : row + 1, :lanes]
            above = values[blocks * tile : (blocks + 1) * tile, :lanes]
            place = t % per_block
            pair = pltpu.roll(above, place * nodes_y, 1) + pair if place else above
            if place == per_block - 1:
                at = t // per_block * tile
                third[at : at + tile] = pair
            ghost = values[:, lanes:]
            if t:
                ghost = pltpu.roll(ghost, t, 1)
            packed = ghost if packed is None else packed + ghost
        if c == CHUNKS - 1:
            for q in range(blocks):
                main[q, subs * tile : (subs + 1) * tile] = packed[q * tile : (q + 1) * tile]
            at = subs // per_block * tile
            third[at : at + tile] = packed[blocks * tile : (blocks + 1) * tile]
            for q in range(blocks + 1):
                row = (blocks + 1) * tile + q
                edge[q, subs : subs + 1] = packed[row : row + 1]
        if c == 0:
            count = blocks + has_next_z.astype(jnp.int32)
            count = count * jnp.where(has_next_x, 2, 1)
            count = count - jnp.logical_or(own, third_here).astype(jnp.int32)
            pl.semaphore_wait(barrier, count)
        each_main(c, lambda copy: copy.start())
    each_edge(lambda copy: copy.start())

    @pl.when(own)
    def _():
        got_main[gy] = main[gz]

    @pl.when(third_here)
    def _():
        got_third[gy] = third[...]

    for s in range(ny):

        @pl.when(jnp.logical_not(jnp.logical_and(own, gy == s)))
        def _(s=s):
            for c in range(CHUNKS):
                pltpu.make_async_remote_copy(
                    src_ref=main.at[0, part(c)],
                    dst_ref=got_main.at[s, part(c)],
                    send_sem=send_main.at[0, c],
                    recv_sem=recv_main.at[s, c],
                    device_id=(gx, gy, gz),
                    device_id_type=MESH,
                ).wait_recv()

    @pl.when(from_third)
    def _():
        for s in range(ny):

            @pl.when(jnp.logical_not(jnp.logical_and(gy == 1, jnp.logical_and(gz == 0, s == gy)) & (gz == gy - 1)))
            def _(s=s):
                for c in range(CHUNKS):
                    pltpu.make_async_remote_copy(
                        src_ref=third.at[third_part(c)],
                        dst_ref=got_third.at[s, third_part(c)],
                        send_sem=send_main.at[0, c],
                        recv_sem=recv_third.at[s, c],
                        device_id=(gx, gy, gz),
                        device_id_type=MESH,
                    ).wait_recv()

            first_block = iota((tile, lanes), 1) // nodes_y % per_block == 0
            for t in range(subs):
                at = t // per_block * tile
                moved = got_third[s, at : at + tile]
                place = t % per_block
                if place:
                    moved = pltpu.roll(moved, lanes - place * nodes_y, 1)
                rows_t = pl.ds(t * tile, tile)
                got_main[s, rows_t] = got_main[s, rows_t] + jnp.where(first_block, moved, 0.0)
            at = subs // per_block * tile
            rows_t = pl.ds(subs * tile, tile)
            got_main[s, rows_t] = got_main[s, rows_t] + got_third[s, at : at + tile]

    def add_edge(source, sem, s):
        pltpu.make_async_remote_copy(
            src_ref=edge.at[0],
            dst_ref=source.at[s],
            send_sem=send_edge.at[0],
            recv_sem=sem.at[s],
            device_id=(gx, gy, gz),
            device_id_type=MESH,
        ).wait_recv()
        for t in range(subs + 1):
            at = pl.ds(t * tile, 1)
            got_main[s, at] = got_main[s, at] + source[s, t : t + 1]

    @pl.when(from_first)
    def _():
        for s in range(ny):
            add_edge(got_first, recv_first, s)

    @pl.when(from_corner)
    def _():
        for s in range(ny):
            add_edge(got_corner, recv_corner, s)

    for copy in fetches[6:]:
        copy.wait()
    lane = iota((tile, lanes), 1)
    lane_y = iota((tile, all_y), 1)
    ghosts = [got_main[s, subs * tile : (subs + 1) * tile] for s in range(ny - 1)]
    bound = [troponin[:, k, :] for k in range(per_block)]
    active = [tension[:, k, :] for k in range(per_block)]
    unbind_rate = [unbind[:, k, :] for k in range(per_block)]
    relax_rate = [relax[:, k, :] for k in range(per_block)]
    for t in range(subs):
        pieces = []
        for s in range(ny):
            value = got_main[s, t * tile : (t + 1) * tile]
            if s:
                moved = pltpu.roll(ghosts[s - 1], lanes - t, 1) if t else ghosts[s - 1]
                value = value + jnp.where(lane % nodes_y == 0, moved, 0.0)
            pieces.append(value)

        def drive(f, k):
            at = (f * per_block + k) * nodes_y
            total = None
            for s in range(ny):
                shift = (s * nodes_y - at) % lanes
                moved = pltpu.roll(pieces[s], shift, 1) if shift else pieces[s]
                total = moved if total is None else jnp.where(lane_y // nodes_y == s, moved, total)
            return total

        for k in range(per_block):
            squared = drive(0, k)
            squared = squared * squared
            binding = squared / (squared + half_square)
            bound[k] = bound[k] + step_size * (
                bind_rate * binding * (1.0 - bound[k]) - unbind_rate[k] * bound[k]
            )
            active[k] = active[k] + step_size * relax_rate[k] * (
                peak_tension * drive(1, k) * bound[k] - active[k]
            )
    for k in range(per_block):
        out_bound[:, k, :] = bound[k]
        out_active[:, k, :] = active[k]

    for c in range(CHUNKS):
        each_main(c, lambda copy: copy.wait_send())
    each_edge(lambda copy: copy.wait_send())


def store_results(bound, active, out_bound, out_active, sem):
    copies = (
        pltpu.make_async_copy(bound, out_bound, sem.at[0]),
        pltpu.make_async_copy(active, out_active, sem.at[1]),
    )
    for copy in copies:
        copy.start()
    for copy in copies:
        copy.wait()


def per_device(calcium, activation, e1, o1, e2, o2, e3, o3, troponin, tension, unbind, relax, *, sizes):
    nx, ny, nz = sizes
    subs, rows, depth, cols = calcium.shape
    nodes_x, per_block, all_y = troponin.shape
    lanes = 2 * per_block * (all_y // ny)
    blocks = nz
    long = (subs + 1) * nodes_x
    short = (subs // per_block + 1) * nodes_x
    vmem = pl.BlockSpec(memory_space=pltpu.VMEM)
    hbm = pl.BlockSpec(memory_space=pltpu.MemorySpace.HBM)
    dma = pltpu.SemaphoreType.DMA
    flat = [x.reshape(1, -1) for x in (e1, o1, e2, o2, e3, o3)]
    shape = jax.ShapeDtypeStruct(troponin.shape, f32)
    operands = [
        pltpu.with_memory_space_constraint(x, pltpu.MemorySpace.HBM)
        for x in (calcium, activation, *flat, troponin, tension, unbind, relax)
    ]
    results = pl.pallas_call(
        functools.partial(kernel, sizes=sizes),
        out_shape=(shape, shape),
        in_specs=[hbm] * 12,
        out_specs=(vmem, vmem),
        scratch_shapes=[
            pltpu.VMEM(calcium.shape, f32),
            pltpu.VMEM(calcium.shape, f32),
            *[pltpu.VMEM(x.shape, x.dtype) for x in (*flat, troponin, tension, unbind, relax)],
            pltpu.VMEM((blocks, long, lanes), f32),
            pltpu.VMEM((short, lanes), f32),
            pltpu.VMEM((blocks + 1, subs + 1, lanes), f32),
            pltpu.VMEM((ny, long, lanes), f32),
            pltpu.VMEM((ny, short, lanes), f32),
            pltpu.VMEM((ny, subs + 1, lanes), f32),
            pltpu.VMEM((ny, subs + 1, lanes), f32),
            dma((2, subs)),
            dma((10,)),
            dma((blocks + 1, CHUNKS)),
            dma((blocks + 1,)),
            dma((ny, CHUNKS)),
            dma((ny, CHUNKS)),
            dma((ny,)),
            dma((ny,)),
        ],
        compiler_params=pltpu.CompilerParams(
            collective_id=0, has_side_effects=True, vmem_limit_bytes=32 * 1024 * 1024
        ),
        name="restrict_steps",
    )(*operands)
    results = [pltpu.with_memory_space_constraint(x, pltpu.MemorySpace.VMEM) for x in results]
    return pl.pallas_call(
        store_results,
        out_shape=(shape, shape),
        in_specs=[vmem] * 2,
        out_specs=(hbm, hbm),
        scratch_shapes=[dma((2,))],
        name="store_results",
    )(*results)


def solution(mesh):
    sizes = tuple(mesh.shape[name] for name in ("gx", "gy", "gz"))
    field = P(None, "gx", "gz", "gy")
    nodes = P("gx", ("gy", "gz"), None)
    return jax.shard_map(
        functools.partial(per_device, sizes=sizes),
        mesh=mesh,
        in_specs=(field, field, P(), P(), P(), P(), P(), P(), nodes, nodes, nodes, nodes),
        out_specs=(nodes, nodes),
        check_vma=False,
    )
```

```python
import functools

import jax
import jax.numpy as jnp
from jax import lax
from jax.experimental import pallas as pl
from jax.experimental.pallas import tpu as pltpu
from jax.sharding import PartitionSpec as P

step_size = 0.2
bind_rate = 2.0
peak_tension = 2.0
half_square = 0.25
f32 = jnp.float32
bf16 = jnp.bfloat16
MESH = pl.DeviceIdType.MESH
CHUNKS = 2


def split(x):
    high = x.astype(bf16)
    return high, (x - high.astype(f32)).astype(bf16)


def node_weights(element, offset, node):
    raw = jnp.where(element == node, 1.0 - offset, 0.0) + jnp.where(
        element + 1 == node, offset, 0.0
    )
    total = jnp.sum(raw, axis=1, keepdims=True)
    return raw, jnp.where(total > 0.0, total, 1.0)


def expand(weight, pick):
    high, low = split(weight)
    return jnp.dot(high, pick, preferred_element_type=f32) + jnp.dot(
        low, pick, preferred_element_type=f32
    )


def iota(shape, dim):
    return lax.broadcasted_iota(jnp.int32, shape, dim)


def kernel(
    calcium,
    activation,
    *refs,
    sizes,
):
    small = refs[:10]
    out_bound, out_active, xc, xa = refs[10:14]
    local = refs[14:24]
    (
        main,
        third,
        edge,
        got_main,
        got_third,
        got_first,
        got_corner,
        relay,
        load_sem,
        small_sem,
        send_main,
        send_edge,
        recv_main,
        recv_third,
        recv_first,
        recv_corner,
        send_relay,
        recv_relay,
    ) = refs[24:]
    e1, o1, e2, o2, e3, o3, troponin, tension, unbind, relax = local
    nx, ny, nz = sizes
    subs, rows, depth, cols = xc.shape
    nodes_x, per_block, all_y = troponin.shape
    nodes_y = all_y // ny
    blocks = nz
    slab = per_block * blocks
    gx, gy, gz = lax.axis_index("gx"), lax.axis_index("gy"), lax.axis_index("gz")
    chunk = subs // CHUNKS

    def load(t):
        return (
            pltpu.make_async_copy(calcium.at[t], xc.at[t], load_sem.at[0, t]),
            pltpu.make_async_copy(activation.at[t], xa.at[t], load_sem.at[1, t]),
        )

    fetches = [
        pltpu.make_async_copy(source, target, small_sem.at[i])
        for i, (source, target) in enumerate(zip(small, local))
    ]
    for copy in fetches:
        copy.start()
    for t in range(subs):
        for copy in load(t):
            copy.start(priority=1)

    barrier = pltpu.get_barrier_semaphore()
    has_next_x = gx + 1 < nx
    has_next_z = gz + 1 < nz
    own = gy == gz
    from_third = jnp.logical_and(gz == 0, gy > 0)
    from_first = gx > 0
    from_corner = jnp.logical_and(from_third, from_first)
    half = blocks // 2
    column = gz // half
    home = gy // half
    last = gz % half == half - 1
    crossing = column != home

    def hello(*device):
        pl.semaphore_signal(barrier, inc=1, device_id=device, device_id_type=MESH)

    def far_slabs(do):
        for i in range(half):
            slab_i = (1 - column) * half + i

            @pl.when(jnp.logical_and(last, slab_i != gy))
            def _(i=i, slab_i=slab_i):
                do(i, slab_i)

    far_slabs(lambda i, slab_i: hello(gx, gy, slab_i))
    for s in range(ny):

        def greet(dx, dz, s=s):
            pl.semaphore_signal(
                barrier, inc=1, device_id=(gx - dx, s, gy - dz), device_id_type=MESH
            )

        @pl.when(jnp.logical_and(jnp.logical_not(crossing), jnp.logical_not(jnp.logical_and(s == gy, own))))
        def _():
            greet(0, 0)

        @pl.when(jnp.logical_and(crossing, s == gy))
        def _():
            greet(0, 0)

        @pl.when(jnp.logical_and(crossing, s != gy))
        def _(s=s):
            hello(gx, s, column * half + half - 1)

        @pl.when(jnp.logical_and(from_third, jnp.logical_not(jnp.logical_and(s == gy, gy - 1 == gz))))
        def _():
            greet(0, 1)

        @pl.when(from_first)
        def _():
            greet(1, 0)

        @pl.when(from_corner)
        def _():
            greet(1, 1)

    for copy in fetches[:6]:
        copy.wait()
    row_count = (slab + 1) * nodes_x + 16
    r = iota((row_count, 1), 0)
    inner = r < (slab + 1) * nodes_x
    tail = r - (slab + 1) * nodes_x
    node_a = jnp.where(inner, r % nodes_x, nodes_x)
    node_b = jnp.where(inner, r // nodes_x, per_block * (tail % 8) + tail // 8)
    raw, total = node_weights(e1[...], o1[...], node_a + gx * nodes_x)
    wide = rows * depth
    pick = (
        iota((raw.shape[1], wide), 0) == gx * rows + iota((raw.shape[1], wide), 1) // depth
    ).astype(bf16)
    weight_x = expand(raw / total, pick)
    raw, total = node_weights(e3[...], o3[...], node_b + gz * slab)
    pick = (
        iota((raw.shape[1], wide), 0) == gz * depth + iota((raw.shape[1], wide), 1) % depth
    ).astype(bf16)
    weight_z = expand(raw / total, pick)
    k_high, k_low = split(weight_x * weight_z)
    k_both = jnp.concatenate([k_high, k_low], axis=0)

    lanes = 2 * per_block * nodes_y
    n = iota((lanes, 1), 0)
    mine = pl.ds(pl.multiple_of(gy * cols, cols), cols)
    spread = []
    for ghost in range(2):
        node = gy * nodes_y + (nodes_y if ghost else n % nodes_y)
        node = node + jnp.zeros_like(n)
        total = node_weights(e2[...], o2[...], node)[1]
        weight = node_weights(e2[:, mine], o2[:, mine], node)[0] / total
        if ghost:
            weight = jnp.where(n % nodes_y == 0, weight, 0.0)
        spread.append(
            jnp.concatenate(
                [
                    jnp.where(n // nodes_y == f * per_block + b, weight, 0.0)
                    for b in range(per_block)
                    for f in range(2)
                ],
                axis=1,
            )
        )
    y_high, y_low = split(jnp.concatenate(spread, axis=0))

    def to_message(values):
        high, low = split(values)
        dims = (((1,), (1,)), ((), ()))
        dot = functools.partial(
            lax.dot_general, dimension_numbers=dims, preferred_element_type=f32
        )
        return dot(high, y_high) + dot(low, y_high) + dot(high, y_low)

    def part(c):
        first = c * chunk * nodes_x
        last = (c + 1) * chunk * nodes_x + (nodes_x if c == CHUNKS - 1 else 0)
        return pl.ds(first, last - first)

    def main_copy(q, c):
        return pltpu.make_async_remote_copy(
            src_ref=main.at[q, part(c)],
            dst_ref=got_main.at[gy, part(c)],
            send_sem=send_main.at[q, c],
            recv_sem=recv_main.at[gy, c],
            device_id=(gx, gz, q),
            device_id_type=MESH,
        )

    def hand_over(q, c):
        return pltpu.make_async_remote_copy(
            src_ref=main.at[q, part(c)],
            dst_ref=relay.at[gz % half, q % half, part(c)],
            send_sem=send_main.at[q, c],
            recv_sem=recv_relay.at[gz % half, q % half, c],
            device_id=(gx, gy, q // half * half + half - 1),
            device_id_type=MESH,
        )

    def forward(i, slab_i, j, c):
        return pltpu.make_async_remote_copy(
            src_ref=relay.at[i, j, part(c)],
            dst_ref=got_main.at[gy, part(c)],
            send_sem=send_relay.at[i, j, c],
            recv_sem=recv_main.at[gy, c],
            device_id=(gx, slab_i, column * half + j),
            device_id_type=MESH,
        )

    def third_part(c):
        step = chunk // per_block * nodes_x
        return pl.ds(c * step, step + (nodes_x if c == CHUNKS - 1 else 0))

    def third_copy(c):
        return pltpu.make_async_remote_copy(
            src_ref=third.at[third_part(c)],
            dst_ref=got_third.at[gy, third_part(c)],
            send_sem=send_main.at[blocks, c],
            recv_sem=recv_third.at[gy, c],
            device_id=(gx, gz + 1, 0),
            device_id_type=MESH,
        )

    def first_copy(q):
        return pltpu.make_async_remote_copy(
            src_ref=edge.at[q],
            dst_ref=got_first.at[gy],
            send_sem=send_edge.at[q],
            recv_sem=recv_first.at[gy],
            device_id=(gx + 1, gz, q),
            device_id_type=MESH,
        )

    def corner_copy():
        return pltpu.make_async_remote_copy(
            src_ref=edge.at[blocks],
            dst_ref=got_corner.at[gy],
            send_sem=send_edge.at[blocks],
            recv_sem=recv_corner.at[gy],
            device_id=(gx + 1, gz + 1, 0),
            device_id_type=MESH,
        )

    third_here = jnp.logical_and(gz == 0, gy == 1)
    third_away = jnp.logical_and(has_next_z, jnp.logical_not(third_here))

    def each_main(c, do):
        for q in range(blocks):

            @pl.when(jnp.where(own, gz != q, column == q // half))
            def _(q=q):
                do(main_copy(q, c))

            @pl.when(jnp.logical_and(jnp.logical_not(own), column != q // half))
            def _(q=q):
                do(hand_over(q, c))

        @pl.when(third_away)
        def _():
            do(third_copy(c))

    def each_edge(do):
        @pl.when(has_next_x)
        def _():
            for q in range(blocks):
                do(first_copy(q))

        @pl.when(jnp.logical_and(has_next_x, has_next_z))
        def _():
            do(corner_copy())

    packed = pair = None
    tile = nodes_x
    for c in range(CHUNKS):
        gathered = []
        for t in range(c * chunk, (c + 1) * chunk):
            for copy in load(t):
                copy.wait()
            field = jnp.concatenate(
                [xc[t].reshape(wide, cols), xa[t].reshape(wide, cols)], axis=1
            )
            high, low = split(field)
            both = jnp.dot(k_both, high, preferred_element_type=f32)
            node = (
                both[:row_count]
                + both[row_count:]
                + jnp.dot(k_high, low, preferred_element_type=f32)
            )
            sides = []
            for k in range(per_block):
                pieces = []
                for q in range(blocks + 1):
                    b = q * per_block + k
                    if b <= slab:
                        pieces.append(node[b * tile : (b + 1) * tile])
                    else:
                        pieces.append(jnp.zeros((tile, 2 * cols), f32))
                base = (slab + 1) * tile + 8 * k
                pieces.append(node[base : base + 8])
                sides.append(jnp.concatenate(pieces, axis=0))
            gathered.append(jnp.concatenate(sides, axis=1))
        result = to_message(jnp.concatenate(gathered, axis=0))
        per = (blocks + 1) * tile + 8
        for k, t in enumerate(range(c * chunk, (c + 1) * chunk)):
            values = result[k * per : (k + 1) * per]
            for q in range(blocks):
                main[q, t * tile : (t + 1) * tile] = values[q * tile : (q + 1) * tile, :lanes]
            for q in range(blocks + 1):
                row = (blocks + 1) * tile + q
                edge[q, t : t + 1] = values[row : row + 1, :lanes]
            above = values[blocks * tile : (blocks + 1) * tile, :lanes]
            place = t % per_block
            pair = pltpu.roll(above, place * nodes_y, 1) + pair if place else above
            if place == per_block - 1:
                at = t // per_block * tile
                third[at : at + tile] = pair
            ghost = values[:, lanes:]
            if t:
                ghost = pltpu.roll(ghost, t, 1)
            packed = ghost if packed is None else packed + ghost
        if c == CHUNKS - 1:
            for q in range(blocks):
                main[q, subs * tile : (subs + 1) * tile] = packed[q * tile : (q + 1) * tile]
            at = subs // per_block * tile
            third[at : at + tile] = packed[blocks * tile : (blocks + 1) * tile]
            for q in range(blocks + 1):
                row = (blocks + 1) * tile + q
                edge[q, subs : subs + 1] = packed[row : row + 1]
        if c == 0:
            extra = blocks + has_next_z.astype(jnp.int32)
            count = jnp.where(has_next_x, extra, 0)
            count = count + jnp.where(own, blocks - 1, half + 1)
            count = count + third_away.astype(jnp.int32)
            served = half - crossing.astype(jnp.int32)
            count = count + jnp.where(last, served * half, 0)
            pl.semaphore_wait(barrier, count)
        each_main(c, lambda copy: copy.start())
    each_edge(lambda copy: copy.start())

    def pass_on(c):
        def one(i, slab_i):
            for j in range(half):
                pltpu.make_async_remote_copy(
                    src_ref=main.at[0, part(c)],
                    dst_ref=relay.at[i, j, part(c)],
                    send_sem=send_main.at[0, c],
                    recv_sem=recv_relay.at[i, j, c],
                    device_id=(gx, gy, gz),
                    device_id_type=MESH,
                ).wait_recv()
                forward(i, slab_i, j, c).start()

        far_slabs(one)

    for c in range(CHUNKS):
        pass_on(c)

    @pl.when(own)
    def _():
        got_main[gy] = main[gz]

    @pl.when(third_here)
    def _():
        got_third[gy] = third[...]

    for s in range(ny):

        @pl.when(jnp.logical_not(jnp.logical_and(own, gy == s)))
        def _(s=s):
            for c in range(CHUNKS):
                pltpu.make_async_remote_copy(
                    src_ref=main.at[0, part(c)],
                    dst_ref=got_main.at[s, part(c)],
                    send_sem=send_main.at[0, c],
                    recv_sem=recv_main.at[s, c],
                    device_id=(gx, gy, gz),
                    device_id_type=MESH,
                ).wait_recv()

    @pl.when(from_third)
    def _():
        for s in range(ny):

            @pl.when(jnp.logical_not(jnp.logical_and(gy == 1, jnp.logical_and(gz == 0, s == gy)) & (gz == gy - 1)))
            def _(s=s):
                for c in range(CHUNKS):
                    pltpu.make_async_remote_copy(
                        src_ref=third.at[third_part(c)],
                        dst_ref=got_third.at[s, third_part(c)],
                        send_sem=send_main.at[0, c],
                        recv_sem=recv_third.at[s, c],
                        device_id=(gx, gy, gz),
                        device_id_type=MESH,
                    ).wait_recv()

            first_block = iota((tile, lanes), 1) // nodes_y % per_block == 0
            for t in range(subs):
                at = t // per_block * tile
                moved = got_third[s, at : at + tile]
                place = t % per_block
                if place:
                    moved = pltpu.roll(moved, lanes - place * nodes_y, 1)
                rows_t = pl.ds(t * tile, tile)
                got_main[s, rows_t] = got_main[s, rows_t] + jnp.where(first_block, moved, 0.0)
            at = subs // per_block * tile
            rows_t = pl.ds(subs * tile, tile)
            got_main[s, rows_t] = got_main[s, rows_t] + got_third[s, at : at + tile]

    def add_edge(source, sem, s):
        pltpu.make_async_remote_copy(
            src_ref=edge.at[0],
            dst_ref=source.at[s],
            send_sem=send_edge.at[0],
            recv_sem=sem.at[s],
            device_id=(gx, gy, gz),
            device_id_type=MESH,
        ).wait_recv()
        for t in range(subs + 1):
            at = pl.ds(t * tile, 1)
            got_main[s, at] = got_main[s, at] + source[s, t : t + 1]

    @pl.when(from_first)
    def _():
        for s in range(ny):
            add_edge(got_first, recv_first, s)

    @pl.when(from_corner)
    def _():
        for s in range(ny):
            add_edge(got_corner, recv_corner, s)

    for copy in fetches[6:]:
        copy.wait()
    lane = iota((tile, lanes), 1)
    lane_y = iota((tile, all_y), 1)
    ghosts = [got_main[s, subs * tile : (subs + 1) * tile] for s in range(ny - 1)]
    bound = [troponin[:, k, :] for k in range(per_block)]
    active = [tension[:, k, :] for k in range(per_block)]
    unbind_rate = [unbind[:, k, :] for k in range(per_block)]
    relax_rate = [relax[:, k, :] for k in range(per_block)]
    for t in range(subs):
        pieces = []
        for s in range(ny):
            value = got_main[s, t * tile : (t + 1) * tile]
            if s:
                moved = pltpu.roll(ghosts[s - 1], lanes - t, 1) if t else ghosts[s - 1]
                value = value + jnp.where(lane % nodes_y == 0, moved, 0.0)
            pieces.append(value)

        def drive(f, k):
            at = (f * per_block + k) * nodes_y
            total = None
            for s in range(ny):
                shift = (s * nodes_y - at) % lanes
                moved = pltpu.roll(pieces[s], shift, 1) if shift else pieces[s]
                total = moved if total is None else jnp.where(lane_y // nodes_y == s, moved, total)
            return total

        for k in range(per_block):
            squared = drive(0, k)
            squared = squared * squared
            binding = squared / (squared + half_square)
            bound[k] = bound[k] + step_size * (
                bind_rate * binding * (1.0 - bound[k]) - unbind_rate[k] * bound[k]
            )
            active[k] = active[k] + step_size * relax_rate[k] * (
                peak_tension * drive(1, k) * bound[k] - active[k]
            )
    for k in range(per_block):
        out_bound[:, k, :] = bound[k]
        out_active[:, k, :] = active[k]

    for c in range(CHUNKS):
        each_main(c, lambda copy: copy.wait_send())
        def sent(i, slab_i, c=c):
            for j in range(half):
                forward(i, slab_i, j, c).wait_send()

        far_slabs(sent)
    each_edge(lambda copy: copy.wait_send())


def store_results(bound, active, out_bound, out_active, sem):
    copies = (
        pltpu.make_async_copy(bound, out_bound, sem.at[0]),
        pltpu.make_async_copy(active, out_active, sem.at[1]),
    )
    for copy in copies:
        copy.start()
    for copy in copies:
        copy.wait()


def per_device(calcium, activation, e1, o1, e2, o2, e3, o3, troponin, tension, unbind, relax, *, sizes):
    nx, ny, nz = sizes
    subs, rows, depth, cols = calcium.shape
    nodes_x, per_block, all_y = troponin.shape
    lanes = 2 * per_block * (all_y // ny)
    blocks = nz
    long = (subs + 1) * nodes_x
    short = (subs // per_block + 1) * nodes_x
    vmem = pl.BlockSpec(memory_space=pltpu.VMEM)
    hbm = pl.BlockSpec(memory_space=pltpu.MemorySpace.HBM)
    dma = pltpu.SemaphoreType.DMA
    flat = [x.reshape(1, -1) for x in (e1, o1, e2, o2, e3, o3)]
    shape = jax.ShapeDtypeStruct(troponin.shape, f32)
    operands = [
        pltpu.with_memory_space_constraint(x, pltpu.MemorySpace.HBM)
        for x in (calcium, activation, *flat, troponin, tension, unbind, relax)
    ]
    results = pl.pallas_call(
        functools.partial(kernel, sizes=sizes),
        out_shape=(shape, shape),
        in_specs=[hbm] * 12,
        out_specs=(vmem, vmem),
        scratch_shapes=[
            pltpu.VMEM(calcium.shape, f32),
            pltpu.VMEM(calcium.shape, f32),
            *[pltpu.VMEM(x.shape, x.dtype) for x in (*flat, troponin, tension, unbind, relax)],
            pltpu.VMEM((blocks, long, lanes), f32),
            pltpu.VMEM((short, lanes), f32),
            pltpu.VMEM((blocks + 1, subs + 1, lanes), f32),
            pltpu.VMEM((ny, long, lanes), f32),
            pltpu.VMEM((ny, short, lanes), f32),
            pltpu.VMEM((ny, subs + 1, lanes), f32),
            pltpu.VMEM((ny, subs + 1, lanes), f32),
            pltpu.VMEM((blocks // 2, blocks // 2, long, lanes), f32),
            dma((2, subs)),
            dma((10,)),
            dma((blocks + 1, CHUNKS)),
            dma((blocks + 1,)),
            dma((ny, CHUNKS)),
            dma((ny, CHUNKS)),
            dma((ny,)),
            dma((ny,)),
            dma((blocks // 2, blocks // 2, CHUNKS)),
            dma((blocks // 2, blocks // 2, CHUNKS)),
        ],
        compiler_params=pltpu.CompilerParams(
            collective_id=0, has_side_effects=True, vmem_limit_bytes=32 * 1024 * 1024
        ),
        name="restrict_steps",
    )(*operands)
    results = [pltpu.with_memory_space_constraint(x, pltpu.MemorySpace.VMEM) for x in results]
    return pl.pallas_call(
        store_results,
        out_shape=(shape, shape),
        in_specs=[vmem] * 2,
        out_specs=(hbm, hbm),
        scratch_shapes=[dma((2,))],
        name="store_results",
    )(*results)


def solution(mesh):
    sizes = tuple(mesh.shape[name] for name in ("gx", "gy", "gz"))
    field = P(None, "gx", "gz", "gy")
    nodes = P("gx", ("gy", "gz"), None)
    return jax.shard_map(
        functools.partial(per_device, sizes=sizes),
        mesh=mesh,
        in_specs=(field, field, P(), P(), P(), P(), P(), P(), nodes, nodes, nodes, nodes),
        out_specs=(nodes, nodes),
        check_vma=False,
    )
```

```python
import functools

import jax
import jax.numpy as jnp
from jax import lax
from jax.experimental import pallas as pl
from jax.experimental.pallas import tpu as pltpu
from jax.sharding import PartitionSpec as P

step_size = 0.2
bind_rate = 2.0
peak_tension = 2.0
half_square = 0.25
f32 = jnp.float32
bf16 = jnp.bfloat16
MESH = pl.DeviceIdType.MESH


def split(x):
    high = x.astype(bf16)
    return high, (x - high.astype(f32)).astype(bf16)


def node_weights(element, offset, node):
    raw = jnp.where(element == node, 1.0 - offset, 0.0) + jnp.where(
        element + 1 == node, offset, 0.0
    )
    total = jnp.sum(raw, axis=1, keepdims=True)
    return raw, jnp.where(total > 0.0, total, 1.0)


def expand(weight, pick):
    high, low = split(weight)
    return jnp.dot(high, pick, preferred_element_type=f32) + jnp.dot(
        low, pick, preferred_element_type=f32
    )


def iota(shape, dim):
    return lax.broadcasted_iota(jnp.int32, shape, dim)


def kernel(
    calcium,
    activation,
    *refs,
    sizes,
):
    small = refs[:10]
    out_bound, out_active, x = refs[10:13]
    local = refs[13:23]
    (
        main,
        third,
        edge,
        got_main,
        got_third,
        got_edge,
        pool,
        send_relay,
        recv_main,
        recv_third,
        recv_edge,
    ) = refs[23:]
    e1, o1, e2, o2, e3, o3, troponin, tension, unbind, relax = local
    nx, ny, nz = sizes
    _, subs, rows, depth, cols = x.shape
    nodes_x, per_block, all_y = troponin.shape
    nodes_y = all_y // ny
    blocks = nz
    slab = per_block * blocks
    gx, gy, gz = lax.axis_index("gx"), lax.axis_index("gy"), lax.axis_index("gz")
    groups = [[t, t + 1] for t in range(0, subs, 2)]
    cuts = [group[-1] + 1 for group in groups]
    chunks = len(cuts)

    def load(t):
        at = len(small) + t
        return [
            pltpu.make_async_copy(field.at[t], x.at[f, t], pool.at[at])
            for f, field in enumerate((calcium, activation))
        ]

    def loaded(t):
        at = len(small) + t
        pltpu.make_async_copy(calcium.at[pl.ds(0, 2)], x.at[:, t], pool.at[at]).wait()

    fetches = [
        pltpu.make_async_copy(source, target, pool.at[i])
        for i, (source, target) in enumerate(zip(small, local))
    ]
    for copy in fetches:
        copy.start()
    for t in range(subs):
        for copy in load(t):
            copy.start(priority=1)

    barrier = pltpu.get_barrier_semaphore()
    has_next_x = gx + 1 < nx
    has_next_z = gz + 1 < nz
    own = gy == gz
    from_third = jnp.logical_and(gz == 0, gy > 0)
    from_first = gx > 0
    from_corner = jnp.logical_and(from_third, from_first)
    half = blocks // 2
    column = gz // half
    home = gy // half
    last = gz % half == half - 1
    crossing = column != home

    def hello(*device):
        pl.semaphore_signal(barrier, inc=1, device_id=device, device_id_type=MESH)

    def far_slabs(do):
        for i in range(half):
            slab_i = (1 - column) * half + i

            @pl.when(jnp.logical_and(last, slab_i != gy))
            def _(i=i, slab_i=slab_i):
                do(i, slab_i)

    far_slabs(lambda i, slab_i: hello(gx, gy, slab_i))
    for s in range(ny):

        def greet(dx, dz, s=s):
            pl.semaphore_signal(
                barrier, inc=1, device_id=(gx - dx, s, gy - dz), device_id_type=MESH
            )

        @pl.when(jnp.logical_and(jnp.logical_not(crossing), jnp.logical_not(jnp.logical_and(s == gy, own))))
        def _():
            greet(0, 0)

        @pl.when(jnp.logical_and(crossing, s == gy))
        def _():
            greet(0, 0)

        @pl.when(jnp.logical_and(crossing, s != gy))
        def _(s=s):
            hello(gx, s, column * half + half - 1)

        @pl.when(jnp.logical_and(from_third, jnp.logical_not(jnp.logical_and(s == gy, gy - 1 == gz))))
        def _():
            greet(0, 1)

        @pl.when(from_first)
        def _():
            greet(1, 0)

        @pl.when(from_corner)
        def _():
            greet(1, 1)

    for copy in fetches[:6]:
        copy.wait()
    tile = nodes_x
    seg = per_block * nodes_y
    lanes = 2 * seg
    first_side = (blocks + 2) * tile
    other_side = (blocks + 1) * tile
    row_count = first_side + (per_block - 1) * other_side
    r = iota((row_count, 1), 0)
    side = jnp.where(r < first_side, 0, (r - first_side) // other_side + 1)
    place = jnp.where(r < first_side, r, (r - first_side) % other_side)
    inner = place < jnp.where(r < first_side, first_side, other_side) - tile
    node_a = jnp.where(inner, place % tile, nodes_x)
    node_b = per_block * jnp.where(inner, place // tile, place % tile) + side
    raw, total = node_weights(e1[...], o1[...], node_a + gx * nodes_x)
    wide = rows * depth
    pick = (
        iota((raw.shape[1], wide), 0) == gx * rows + iota((raw.shape[1], wide), 1) // depth
    ).astype(bf16)
    weight_x = expand(raw / total, pick)
    raw, total = node_weights(e3[...], o3[...], node_b + gz * slab)
    pick = (
        iota((raw.shape[1], wide), 0) == gz * depth + iota((raw.shape[1], wide), 1) % depth
    ).astype(bf16)
    weight_z = expand(raw / total, pick)
    k_high, k_low = split(weight_x * weight_z)
    k_both = jnp.concatenate([k_high, k_low], axis=0)

    def y_weights():
        n = iota((lanes, 1), 0)
        mine = pl.ds(pl.multiple_of(gy * cols, cols), cols)
        spot = n % seg
        beyond = jnp.logical_and(spot >= nodes_y, spot % subs == nodes_y % subs)
        beyond = jnp.logical_and(beyond, spot < nodes_y + per_block * subs)
        node = gy * nodes_y + jnp.where(spot < nodes_y, spot, nodes_y)
        total = node_weights(e2[...], o2[...], node)[1]
        weight = node_weights(e2[:, mine], o2[:, mine], node)[0] / total
        weight = jnp.where(jnp.logical_or(spot < nodes_y, beyond), weight, 0.0).T
        field = iota(weight.shape, 1) // seg
        weight = jnp.concatenate([jnp.where(field == f, weight, 0.0) for f in range(2)], axis=0)
        return jnp.concatenate(split(weight), axis=1)

    def to_message(node, y_both):
        count = node.shape[0]
        out = jnp.dot(
            jnp.concatenate(split(node), axis=0), y_both, preferred_element_type=f32
        )
        return out[:count, :lanes] + out[:count, lanes:] + out[count:, :lanes]

    def span(first, last):
        stop = last * tile + (tile if last == subs else 0)
        return pl.ds(first * tile, stop - first * tile)

    def part(c):
        return span(cuts[c - 1] if c else 0, cuts[c])

    def main_copy(q, c):
        where = part(c) if c < chunks else span(0, subs)
        direct = jnp.logical_or(own, column == q // half).astype(jnp.int32)
        over = 1 - direct
        slot = gz % half * half + q % half
        return pltpu.make_async_remote_copy(
            src_ref=main.at[q, where],
            dst_ref=got_main.at[direct * gy + over * (ny + slot), where],
            send_sem=pool.at[q],
            recv_sem=recv_main.at[direct * gy + over * (ny + slot * chunks + c % chunks)],
            device_id=(
                gx,
                direct * gz + over * gy,
                direct * q + over * (q // half * half + half - 1),
            ),
            device_id_type=MESH,
        )

    def forward(i, slab_i, j, c):
        where = part(c) if c < chunks else span(0, subs)
        return pltpu.make_async_remote_copy(
            src_ref=got_main.at[ny + i * half + j, where],
            dst_ref=got_main.at[gy, where],
            send_sem=send_relay.at[i, j],
            recv_sem=recv_main.at[gy],
            device_id=(gx, slab_i, column * half + j),
            device_id_type=MESH,
        )

    def third_copy(where):
        return pltpu.make_async_remote_copy(
            src_ref=third.at[where],
            dst_ref=got_third.at[gy, where],
            send_sem=pool.at[blocks],
            recv_sem=recv_third.at[gy],
            device_id=(gx, gz + 1, 0),
            device_id_type=MESH,
        )

    def edge_copy(q, corner):
        return pltpu.make_async_remote_copy(
            src_ref=edge.at[q],
            dst_ref=got_edge.at[gy, corner],
            send_sem=pool.at[len(small) + q],
            recv_sem=recv_edge.at[gy],
            device_id=(gx + 1, gz + corner, 0 if corner else q),
            device_id_type=MESH,
        )

    third_here = jnp.logical_and(gz == 0, gy == 1)
    third_away = jnp.logical_and(has_next_z, jnp.logical_not(third_here))

    def each_main(do, c, up):
        for q in range(blocks):

            @pl.when(jnp.logical_not(jnp.logical_and(own, gz == q)))
            def _(q=q):
                do(main_copy(q, c))

        if up.size:

            @pl.when(third_away)
            def _():
                do(third_copy(up))

    def send(c):
        pairs = [cut // per_block * tile for cut in (cuts[c - 1] if c else 0, cuts[c])]
        pairs[1] += tile if c == chunks - 1 else 0
        each_main(lambda copy: copy.start(), c, pl.ds(pairs[0], pairs[1] - pairs[0]))

    def each_edge(do):
        @pl.when(has_next_x)
        def _():
            for q in range(blocks):
                do(edge_copy(q, 0))

        @pl.when(jnp.logical_and(has_next_x, has_next_z))
        def _():
            do(edge_copy(blocks, 1))

    spot = iota((tile, lanes), 1) % seg
    pieces = blocks + 2
    state = {"packed": None, "pair": None}

    def nodes_of(group):
        fields = [x[f, t].reshape(wide, cols) for t in group for f in range(2)]
        high, low = split(jnp.concatenate(fields, axis=1))
        both = jnp.dot(k_both, high, preferred_element_type=f32)
        node = (
            both[:row_count]
            + both[row_count:]
            + jnp.dot(k_high, low, preferred_element_type=f32)
        )
        width = 2 * cols
        return jnp.concatenate(
            [node[:, i * width : (i + 1) * width] for i in range(len(group))], axis=0
        )

    def place_message(t, values):
        main_tiles, ghost_tiles = [], []
        for i in range(pieces):
            total, ghost = values[i * tile : (i + 1) * tile], 0.0
            here = total
            for k in range(per_block):
                if k and i == blocks:
                    here = None
                elif k:
                    at = first_side + (k - 1) * other_side + (i - (i > blocks)) * tile
                    here = values[at : at + tile]
                in_place = spot // nodes_y == k
                if k:
                    total = jnp.where(in_place, 0.0 if here is None else pltpu.roll(here, k * nodes_y, 1), total)
                if here is not None:
                    ghost = jnp.where(spot == nodes_y + k * subs, here, ghost)
            main_tiles.append(total)
            ghost_tiles.append(pltpu.roll(ghost, t, 1) if t else ghost)
        for q in range(blocks):
            main[q, t * tile : (t + 1) * tile] = main_tiles[q]
        for q in range(blocks + 1):
            edge[q, t : t + 1] = main_tiles[blocks + 1][q : q + 1]
        above = main_tiles[blocks]
        fold = t % per_block
        state["pair"] = pltpu.roll(above, fold * nodes_y, 1) + state["pair"] if fold else above
        if fold == per_block - 1:
            at = t // per_block * tile
            third[at : at + tile] = state["pair"]
        packed = state["packed"]
        packed = ghost_tiles if packed is None else [x + y for x, y in zip(packed, ghost_tiles)]
        state["packed"] = packed
        if t == subs - 1:
            for q in range(blocks):
                main[q, subs * tile : (subs + 1) * tile] = packed[q]
            at = subs // per_block * tile
            third[at : at + tile] = packed[blocks]
            for q in range(blocks + 1):
                edge[q, subs : subs + 1] = packed[blocks + 1][q : q + 1]

    y_both = node = None
    for g in range(len(groups) + 1):
        group = groups[g] if g < len(groups) else []
        for t in group:
            loaded(t)
        before, node = node, nodes_of(group) if group else None
        if g == 0:
            y_both = y_weights()
            continue
        values = to_message(before, y_both)
        for i, t in enumerate(groups[g - 1]):
            place_message(t, values[i * row_count : (i + 1) * row_count])
        c = g - 1
        if c == 0:
            extra = blocks + has_next_z.astype(jnp.int32)
            count = jnp.where(has_next_x, extra, 0)
            count = count + jnp.where(own, blocks - 1, half + 1)
            count = count + third_away.astype(jnp.int32)
            served = half - crossing.astype(jnp.int32)
            count = count + jnp.where(last, served * half, 0)
            pl.semaphore_wait(barrier, count)
        send(c)
    each_edge(lambda copy: copy.start())

    for copy in fetches[6:]:
        copy.wait()

    def pass_on(i, slab_i):
        for c in range(chunks):
            for j in range(half):
                slot = i * half + j
                pltpu.make_async_remote_copy(
                    src_ref=main.at[0, part(c)],
                    dst_ref=got_main.at[ny + slot, part(c)],
                    send_sem=pool.at[0],
                    recv_sem=recv_main.at[ny + slot * chunks + c],
                    device_id=(gx, gy, gz),
                    device_id_type=MESH,
                ).wait_recv()
                forward(i, slab_i, j, c).start()

    far_slabs(pass_on)

    @pl.when(own)
    def _():
        got_main[gy] = main[gz]

    @pl.when(third_here)
    def _():
        got_third[gy] = third[...]

    for s in range(ny):

        @pl.when(jnp.logical_not(jnp.logical_and(own, gy == s)))
        def _(s=s):
            pltpu.make_async_remote_copy(
                src_ref=main.at[0],
                dst_ref=got_main.at[s],
                send_sem=pool.at[0],
                recv_sem=recv_main.at[s],
                device_id=(gx, gy, gz),
                device_id_type=MESH,
            ).wait_recv()

    @pl.when(from_third)
    def _():
        for s in range(ny):

            @pl.when(jnp.logical_not(jnp.logical_and(gy == 1, jnp.logical_and(gz == 0, s == gy)) & (gz == gy - 1)))
            def _(s=s):
                pltpu.make_async_remote_copy(
                    src_ref=third,
                    dst_ref=got_third.at[s],
                    send_sem=pool.at[0],
                    recv_sem=recv_third.at[s],
                    device_id=(gx, gy, gz),
                    device_id_type=MESH,
                ).wait_recv()

            first_block = iota((tile, lanes), 1) // nodes_y % per_block == 0
            for t in range(subs):
                at = t // per_block * tile
                moved = got_third[s, at : at + tile]
                place = t % per_block
                if place:
                    moved = pltpu.roll(moved, lanes - place * nodes_y, 1)
                rows_t = pl.ds(t * tile, tile)
                got_main[s, rows_t] = got_main[s, rows_t] + jnp.where(first_block, moved, 0.0)
            at = subs // per_block * tile
            rows_t = pl.ds(subs * tile, tile)
            got_main[s, rows_t] = got_main[s, rows_t] + got_third[s, at : at + tile]

    def add_edge(corners):
        for s in range(ny):
            pltpu.make_async_remote_copy(
                src_ref=edge.at[pl.ds(0, 1 + corners)],
                dst_ref=got_edge.at[s, pl.ds(0, 1 + corners)],
                send_sem=pool.at[0],
                recv_sem=recv_edge.at[s],
                device_id=(gx, gy, gz),
                device_id_type=MESH,
            ).wait_recv()
            for t in range(subs + 1):
                at = pl.ds(t * tile, 1)
                total = got_main[s, at]
                for corner in range(1 + corners):
                    total = total + got_edge[s, corner, t : t + 1]
                got_main[s, at] = total

    @pl.when(jnp.logical_and(from_first, jnp.logical_not(from_corner)))
    def _():
        add_edge(0)

    @pl.when(from_corner)
    def _():
        add_edge(1)

    lane = iota((tile, lanes), 1)
    lane_y = iota((tile, all_y), 1)
    ghosts = []
    for s in range(ny - 1):
        raw = got_main[s, subs * tile : (subs + 1) * tile]
        ghost = pltpu.roll(raw, lanes - nodes_y, 1)
        for k in range(1, per_block):
            moved = pltpu.roll(raw, (lanes + k * nodes_y - nodes_y - k * subs) % lanes, 1)
            ghost = jnp.where(spot // nodes_y == k, moved, ghost)
        ghosts.append(ghost)
    bound = [troponin[:, k, :] for k in range(per_block)]
    active = [tension[:, k, :] for k in range(per_block)]
    unbind_rate = [unbind[:, k, :] for k in range(per_block)]
    relax_rate = [relax[:, k, :] for k in range(per_block)]
    for t in range(subs):
        pieces = []
        for s in range(ny):
            value = got_main[s, t * tile : (t + 1) * tile]
            if s:
                moved = pltpu.roll(ghosts[s - 1], lanes - t, 1) if t else ghosts[s - 1]
                value = value + jnp.where(lane % nodes_y == 0, moved, 0.0)
            pieces.append(value)

        def drive(f, k):
            at = (f * per_block + k) * nodes_y
            total = None
            for s in range(ny):
                shift = (s * nodes_y - at) % lanes
                moved = pltpu.roll(pieces[s], shift, 1) if shift else pieces[s]
                total = moved if total is None else jnp.where(lane_y // nodes_y == s, moved, total)
            return total

        for k in range(per_block):
            squared = drive(0, k)
            squared = squared * squared
            binding = squared / (squared + half_square)
            bound[k] = bound[k] + step_size * (
                bind_rate * binding * (1.0 - bound[k]) - unbind_rate[k] * bound[k]
            )
            active[k] = active[k] + step_size * relax_rate[k] * (
                peak_tension * drive(1, k) * bound[k] - active[k]
            )
    for k in range(per_block):
        out_bound[:, k, :] = bound[k]
        out_active[:, k, :] = active[k]

    each_main(lambda copy: copy.wait_send(), chunks, pl.ds(0, third.shape[0]))
    each_edge(lambda copy: copy.wait_send())

    def sent(i, slab_i):
        for j in range(half):
            forward(i, slab_i, j, chunks).wait_send()

    far_slabs(sent)


def store_results(bound, active, out_bound, out_active, sem):
    copies = (
        pltpu.make_async_copy(bound, out_bound, sem.at[0]),
        pltpu.make_async_copy(active, out_active, sem.at[1]),
    )
    for copy in copies:
        copy.start()
    for copy in copies:
        copy.wait()


def per_device(calcium, activation, e1, o1, e2, o2, e3, o3, troponin, tension, unbind, relax, *, sizes):
    nx, ny, nz = sizes
    subs, rows, depth, cols = calcium.shape
    nodes_x, per_block, all_y = troponin.shape
    lanes = 2 * per_block * (all_y // ny)
    blocks = nz
    long = (subs + 1) * nodes_x
    short = (subs // per_block + 1) * nodes_x
    vmem = pl.BlockSpec(memory_space=pltpu.VMEM)
    hbm = pl.BlockSpec(memory_space=pltpu.MemorySpace.HBM)
    dma = pltpu.SemaphoreType.DMA
    flat = [x.reshape(1, -1) for x in (e1, o1, e2, o2, e3, o3)]
    shape = jax.ShapeDtypeStruct(troponin.shape, f32)
    operands = [
        pltpu.with_memory_space_constraint(x, pltpu.MemorySpace.HBM)
        for x in (calcium, activation, *flat, troponin, tension, unbind, relax)
    ]
    results = pl.pallas_call(
        functools.partial(kernel, sizes=sizes),
        out_shape=(shape, shape),
        in_specs=[hbm] * 12,
        out_specs=(vmem, vmem),
        scratch_shapes=[
            pltpu.VMEM((2, *calcium.shape), f32),
            *[pltpu.VMEM(x.shape, x.dtype) for x in (*flat, troponin, tension, unbind, relax)],
            pltpu.VMEM((blocks, long, lanes), f32),
            pltpu.VMEM((short, lanes), f32),
            pltpu.VMEM((blocks + 1, subs + 1, lanes), f32),
            pltpu.VMEM((ny + (blocks // 2) ** 2, long, lanes), f32),
            pltpu.VMEM((ny, short, lanes), f32),
            pltpu.VMEM((ny, 2, subs + 1, lanes), f32),
            dma((10 + subs,)),
            dma((blocks // 2, blocks // 2)),
            dma((ny + (blocks // 2) ** 2 * (subs // 2),)),
            dma((ny,)),
            dma((ny,)),
        ],
        compiler_params=pltpu.CompilerParams(
            collective_id=0, has_side_effects=True, vmem_limit_bytes=32 * 1024 * 1024
        ),
        name="restrict_steps",
    )(*operands)
    results = [pltpu.with_memory_space_constraint(x, pltpu.MemorySpace.VMEM) for x in results]
    return pl.pallas_call(
        store_results,
        out_shape=(shape, shape),
        in_specs=[vmem] * 2,
        out_specs=(hbm, hbm),
        scratch_shapes=[dma((2,))],
        name="store_results",
    )(*results)


def solution(mesh):
    sizes = tuple(mesh.shape[name] for name in ("gx", "gy", "gz"))
    field = P(None, "gx", "gz", "gy")
    nodes = P("gx", ("gy", "gz"), None)
    return jax.shard_map(
        functools.partial(per_device, sizes=sizes),
        mesh=mesh,
        in_specs=(field, field, P(), P(), P(), P(), P(), P(), nodes, nodes, nodes, nodes),
        out_specs=(nodes, nodes),
        check_vma=False,
    )
```

```python
import functools

import jax
import jax.numpy as jnp
from jax import lax
from jax.experimental import pallas as pl
from jax.experimental.pallas import tpu as pltpu
from jax.sharding import PartitionSpec as P

step_size = 0.2
bind_rate = 2.0
peak_tension = 2.0
half_square = 0.25
f32 = jnp.float32
bf16 = jnp.bfloat16
MESH = pl.DeviceIdType.MESH


def split(x):
    high = x.astype(bf16)
    return high, (x - high.astype(f32)).astype(bf16)


def node_weights(element, offset, node):
    raw = jnp.where(element == node, 1.0 - offset, 0.0) + jnp.where(
        element + 1 == node, offset, 0.0
    )
    total = jnp.sum(raw, axis=1, keepdims=True)
    return raw, jnp.where(total > 0.0, total, 1.0)


def expand(weight, pick):
    high, low = split(weight)
    return jnp.dot(high, pick, preferred_element_type=f32) + jnp.dot(
        low, pick, preferred_element_type=f32
    )


def iota(shape, dim):
    return lax.broadcasted_iota(jnp.int32, shape, dim)


def kernel(
    calcium,
    activation,
    *refs,
    sizes,
):
    small = refs[:10]
    out_bound, out_active, x = refs[10:13]
    local = refs[13:23]
    (
        main,
        third,
        edge,
        got_main,
        got_third,
        got_edge,
        pool,
        send_relay,
        recv_main,
        recv_third,
        recv_edge,
    ) = refs[23:]
    e1, o1, e2, o2, e3, o3, troponin, tension, unbind, relax = local
    nx, ny, nz = sizes
    _, subs, rows, depth, cols = x.shape
    nodes_x, per_block, all_y = troponin.shape
    nodes_y = all_y // ny
    blocks = nz
    slab = per_block * blocks
    gx, gy, gz = lax.axis_index("gx"), lax.axis_index("gy"), lax.axis_index("gz")
    groups = [[t, t + 1] for t in range(0, subs, 2)]
    cuts = [group[-1] + 1 for group in groups]
    chunks = len(cuts)

    def load(t):
        at = len(small) + t
        return [
            pltpu.make_async_copy(field.at[t], x.at[f, t], pool.at[at])
            for f, field in enumerate((calcium, activation))
        ]

    def loaded(t):
        at = len(small) + t
        pltpu.make_async_copy(calcium.at[pl.ds(0, 2)], x.at[:, t], pool.at[at]).wait()

    fetches = [
        pltpu.make_async_copy(source, target, pool.at[i])
        for i, (source, target) in enumerate(zip(small, local))
    ]
    for copy in fetches:
        copy.start()
    for t in range(subs):
        for copy in load(t):
            copy.start(priority=1)

    barrier = pltpu.get_barrier_semaphore()
    has_next_x = gx + 1 < nx
    has_next_z = gz + 1 < nz
    own = gy == gz
    from_third = jnp.logical_and(gz == 0, gy > 0)
    from_first = gx > 0
    from_corner = jnp.logical_and(from_third, from_first)
    half = blocks // 2
    column = gz // half
    home = gy // half
    last = gz % half == half - 1
    crossing = column != home

    def hello(*device):
        pl.semaphore_signal(barrier, inc=1, device_id=device, device_id_type=MESH)

    def far_slabs(do):
        for i in range(half):
            slab_i = (1 - column) * half + i

            @pl.when(jnp.logical_and(last, slab_i != gy))
            def _(i=i, slab_i=slab_i):
                do(i, slab_i)

    far_slabs(lambda i, slab_i: hello(gx, gy, slab_i))
    for s in range(ny):

        def greet(dx, dz, s=s):
            pl.semaphore_signal(
                barrier, inc=1, device_id=(gx - dx, s, gy - dz), device_id_type=MESH
            )

        @pl.when(jnp.logical_and(jnp.logical_not(crossing), jnp.logical_not(jnp.logical_and(s == gy, own))))
        def _():
            greet(0, 0)

        @pl.when(jnp.logical_and(crossing, s == gy))
        def _():
            greet(0, 0)

        @pl.when(jnp.logical_and(crossing, s != gy))
        def _(s=s):
            hello(gx, s, column * half + half - 1)

        @pl.when(jnp.logical_and(from_third, jnp.logical_not(jnp.logical_and(s == gy, gy - 1 == gz))))
        def _():
            greet(0, 1)

        @pl.when(from_first)
        def _():
            greet(1, 0)

        @pl.when(from_corner)
        def _():
            greet(1, 1)

    for copy in fetches[:6]:
        copy.wait()
    tile = nodes_x
    seg = per_block * nodes_y
    lanes = 2 * seg
    first_side = (blocks + 2) * tile
    other_side = (blocks + 1) * tile
    row_count = first_side + (per_block - 1) * other_side
    r = iota((row_count, 1), 0)
    side = jnp.where(r < first_side, 0, (r - first_side) // other_side + 1)
    place = jnp.where(r < first_side, r, (r - first_side) % other_side)
    inner = place < jnp.where(r < first_side, first_side, other_side) - tile
    node_a = jnp.where(inner, place % tile, nodes_x)
    node_b = per_block * jnp.where(inner, place // tile, place % tile) + side
    raw, total = node_weights(e1[...], o1[...], node_a + gx * nodes_x)
    wide = rows * depth
    pick = (
        iota((raw.shape[1], wide), 0) == gx * rows + iota((raw.shape[1], wide), 1) // depth
    ).astype(bf16)
    weight_x = expand(raw / total, pick)
    raw, total = node_weights(e3[...], o3[...], node_b + gz * slab)
    pick = (
        iota((raw.shape[1], wide), 0) == gz * depth + iota((raw.shape[1], wide), 1) % depth
    ).astype(bf16)
    weight_z = expand(raw / total, pick)
    k_high, k_low = split(weight_x * weight_z)
    k_both = jnp.concatenate([k_high, k_low], axis=0)

    def y_weights():
        n = iota((lanes, 1), 0)
        mine = pl.ds(pl.multiple_of(gy * cols, cols), cols)
        spot = n % seg
        beyond = jnp.logical_and(spot >= nodes_y, spot % subs == nodes_y % subs)
        beyond = jnp.logical_and(beyond, spot < nodes_y + per_block * subs)
        node = gy * nodes_y + jnp.where(spot < nodes_y, spot, nodes_y)
        total = node_weights(e2[...], o2[...], node)[1]
        weight = node_weights(e2[:, mine], o2[:, mine], node)[0] / total
        weight = jnp.where(jnp.logical_or(spot < nodes_y, beyond), weight, 0.0).T
        field = iota(weight.shape, 1) // seg
        weight = jnp.concatenate([jnp.where(field == f, weight, 0.0) for f in range(2)], axis=0)
        return jnp.concatenate(split(weight), axis=1)

    def to_message(node, y_both):
        count = node.shape[0]
        out = jnp.dot(
            jnp.concatenate(split(node), axis=0), y_both, preferred_element_type=f32
        )
        return out[:count, :lanes] + out[:count, lanes:] + out[count:, :lanes]

    def span(first, last):
        stop = last * tile + (tile if last == subs else 0)
        return pl.ds(first * tile, stop - first * tile)

    def part(c):
        return span(cuts[c - 1] if c else 0, cuts[c])

    def main_copy(q, c):
        where = part(c) if c < chunks else span(0, subs)
        direct = jnp.logical_or(own, column == q // half).astype(jnp.int32)
        over = 1 - direct
        line = gz % half
        slot = line * half + q % half
        return pltpu.make_async_remote_copy(
            src_ref=main.at[q, where],
            dst_ref=got_main.at[direct * gy + over * (ny + slot), where],
            send_sem=pool.at[q],
            recv_sem=recv_main.at[direct * gy + over * (ny + line * chunks + c % chunks)],
            device_id=(
                gx,
                direct * gz + over * gy,
                direct * q + over * (q // half * half + half - 1),
            ),
            device_id_type=MESH,
        )

    def forward(i, slab_i, j, c):
        where = part(c) if c < chunks else span(0, subs)
        return pltpu.make_async_remote_copy(
            src_ref=got_main.at[ny + i * half + j, where],
            dst_ref=got_main.at[gy, where],
            send_sem=send_relay.at[i],
            recv_sem=recv_main.at[gy],
            device_id=(gx, slab_i, column * half + j),
            device_id_type=MESH,
        )

    def third_copy(where):
        return pltpu.make_async_remote_copy(
            src_ref=third.at[where],
            dst_ref=got_third.at[gy, where],
            send_sem=pool.at[blocks],
            recv_sem=recv_third.at[gy],
            device_id=(gx, gz + 1, 0),
            device_id_type=MESH,
        )

    def edge_copy(q, corner):
        return pltpu.make_async_remote_copy(
            src_ref=edge.at[q],
            dst_ref=got_edge.at[gy, corner],
            send_sem=pool.at[len(small) + q],
            recv_sem=recv_edge.at[gy],
            device_id=(gx + 1, gz + corner, 0 if corner else q),
            device_id_type=MESH,
        )

    third_here = jnp.logical_and(gz == 0, gy == 1)
    third_away = jnp.logical_and(has_next_z, jnp.logical_not(third_here))

    def each_main(do, c, up):
        for q in range(blocks):

            @pl.when(jnp.logical_not(jnp.logical_and(own, gz == q)))
            def _(q=q):
                do(main_copy(q, c))

        if up.size:

            @pl.when(third_away)
            def _():
                do(third_copy(up))

    def send(c):
        pairs = [cut // per_block * tile for cut in (cuts[c - 1] if c else 0, cuts[c])]
        pairs[1] += tile if c == chunks - 1 else 0
        each_main(lambda copy: copy.start(), c, pl.ds(pairs[0], pairs[1] - pairs[0]))

    late = jnp.logical_or(gy < gz, gy == 0)

    def meet():
        extra = blocks + has_next_z.astype(jnp.int32)
        count = jnp.where(has_next_x, extra, 0)
        count = count + jnp.where(own, blocks - 1, half + 1)
        count = count + third_away.astype(jnp.int32)
        served = half - crossing.astype(jnp.int32)
        count = count + jnp.where(last, served * half, 0)
        pl.semaphore_wait(barrier, count)

    def each_edge(do):
        @pl.when(has_next_x)
        def _():
            for q in range(blocks):
                do(edge_copy(q, 0))

        @pl.when(jnp.logical_and(has_next_x, has_next_z))
        def _():
            do(edge_copy(blocks, 1))

    spot = iota((tile, lanes), 1) % seg
    pieces = blocks + 2
    state = {"packed": None, "pair": None}

    def nodes_of(group):
        nodes = []
        for t in group:
            high, low = split(
                jnp.concatenate([x[f, t].reshape(wide, cols) for f in range(2)], axis=1)
            )
            both = jnp.dot(k_both, high, preferred_element_type=f32)
            nodes.append(
                both[:row_count]
                + both[row_count:]
                + jnp.dot(k_high, low, preferred_element_type=f32)
            )
        return jnp.concatenate(nodes, axis=0)

    def place_message(t, values):
        main_tiles, ghost_tiles = [], []
        for i in range(pieces):
            total, ghost = values[i * tile : (i + 1) * tile], 0.0
            here = total
            for k in range(per_block):
                if k and i == blocks:
                    here = None
                elif k:
                    at = first_side + (k - 1) * other_side + (i - (i > blocks)) * tile
                    here = values[at : at + tile]
                in_place = spot // nodes_y == k
                if k:
                    total = jnp.where(in_place, 0.0 if here is None else pltpu.roll(here, k * nodes_y, 1), total)
                if here is not None:
                    ghost = jnp.where(spot == nodes_y + k * subs, here, ghost)
            main_tiles.append(total)
            ghost_tiles.append(pltpu.roll(ghost, t, 1) if t else ghost)
        for q in range(blocks):
            main[q, t * tile : (t + 1) * tile] = main_tiles[q]
        for q in range(blocks + 1):
            edge[q, t : t + 1] = main_tiles[blocks + 1][q : q + 1]
        above = main_tiles[blocks]
        fold = t % per_block
        state["pair"] = pltpu.roll(above, fold * nodes_y, 1) + state["pair"] if fold else above
        if fold == per_block - 1:
            at = t // per_block * tile
            third[at : at + tile] = state["pair"]
        packed = state["packed"]
        packed = ghost_tiles if packed is None else [x + y for x, y in zip(packed, ghost_tiles)]
        state["packed"] = packed
        if t == subs - 1:
            for q in range(blocks):
                main[q, subs * tile : (subs + 1) * tile] = packed[q]
            at = subs // per_block * tile
            third[at : at + tile] = packed[blocks]
            for q in range(blocks + 1):
                edge[q, subs : subs + 1] = packed[blocks + 1][q : q + 1]

    y_both = node = None
    for g in range(len(groups) + 1):
        group = groups[g] if g < len(groups) else []
        for t in group:
            loaded(t)
        before, node = node, nodes_of(group) if group else None
        if g == 0:
            y_both = y_weights()
            continue
        values = to_message(before, y_both)
        for i, t in enumerate(groups[g - 1]):
            place_message(t, values[i * row_count : (i + 1) * row_count])
        c = g - 1
        if c < chunks - 2:

            @pl.when(jnp.logical_not(late))
            def _(c=c):
                if c == 0:
                    meet()
                send(c)

            continue
        if c == chunks - 2:

            @pl.when(late)
            def _(c=c):
                meet()
                for before_c in range(c):
                    send(before_c)

        send(c)
    each_edge(lambda copy: copy.start())

    for copy in fetches[6:]:
        copy.wait()

    def pass_on(i, slab_i):
        for c in range(chunks):
            pltpu.make_async_remote_copy(
                src_ref=main.at[pl.ds(0, half), part(c)],
                dst_ref=got_main.at[pl.ds(ny + i * half, half), part(c)],
                send_sem=pool.at[0],
                recv_sem=recv_main.at[ny + i * chunks + c],
                device_id=(gx, gy, gz),
                device_id_type=MESH,
            ).wait_recv()
            for j in range(half):
                forward(i, slab_i, j, c).start()

    far_slabs(pass_on)

    @pl.when(own)
    def _():
        got_main[gy] = main[gz]

    @pl.when(third_here)
    def _():
        got_third[gy] = third[...]

    for s in range(ny):

        @pl.when(jnp.logical_not(jnp.logical_and(own, gy == s)))
        def _(s=s):
            pltpu.make_async_remote_copy(
                src_ref=main.at[0],
                dst_ref=got_main.at[s],
                send_sem=pool.at[0],
                recv_sem=recv_main.at[s],
                device_id=(gx, gy, gz),
                device_id_type=MESH,
            ).wait_recv()

    @pl.when(from_third)
    def _():
        for s in range(ny):

            @pl.when(jnp.logical_not(jnp.logical_and(gy == 1, jnp.logical_and(gz == 0, s == gy)) & (gz == gy - 1)))
            def _(s=s):
                pltpu.make_async_remote_copy(
                    src_ref=third,
                    dst_ref=got_third.at[s],
                    send_sem=pool.at[0],
                    recv_sem=recv_third.at[s],
                    device_id=(gx, gy, gz),
                    device_id_type=MESH,
                ).wait_recv()

            first_block = iota((tile, lanes), 1) // nodes_y % per_block == 0
            for t in range(subs):
                at = t // per_block * tile
                moved = got_third[s, at : at + tile]
                place = t % per_block
                if place:
                    moved = pltpu.roll(moved, lanes - place * nodes_y, 1)
                rows_t = pl.ds(t * tile, tile)
                got_main[s, rows_t] = got_main[s, rows_t] + jnp.where(first_block, moved, 0.0)
            at = subs // per_block * tile
            rows_t = pl.ds(subs * tile, tile)
            got_main[s, rows_t] = got_main[s, rows_t] + got_third[s, at : at + tile]

    def add_edge(corners):
        for s in range(ny):
            pltpu.make_async_remote_copy(
                src_ref=edge.at[pl.ds(0, 1 + corners)],
                dst_ref=got_edge.at[s, pl.ds(0, 1 + corners)],
                send_sem=pool.at[0],
                recv_sem=recv_edge.at[s],
                device_id=(gx, gy, gz),
                device_id_type=MESH,
            ).wait_recv()
            for t in range(subs + 1):
                at = pl.ds(t * tile, 1)
                total = got_main[s, at]
                for corner in range(1 + corners):
                    total = total + got_edge[s, corner, t : t + 1]
                got_main[s, at] = total

    @pl.when(jnp.logical_and(from_first, jnp.logical_not(from_corner)))
    def _():
        add_edge(0)

    @pl.when(from_corner)
    def _():
        add_edge(1)

    lane = iota((tile, lanes), 1)
    lane_y = iota((tile, all_y), 1)
    ghosts = []
    for s in range(ny - 1):
        raw = got_main[s, subs * tile : (subs + 1) * tile]
        ghost = pltpu.roll(raw, lanes - nodes_y, 1)
        for k in range(1, per_block):
            moved = pltpu.roll(raw, (lanes + k * nodes_y - nodes_y - k * subs) % lanes, 1)
            ghost = jnp.where(spot // nodes_y == k, moved, ghost)
        ghosts.append(ghost)
    bound = [troponin[:, k, :] for k in range(per_block)]
    active = [tension[:, k, :] for k in range(per_block)]
    unbind_rate = [unbind[:, k, :] for k in range(per_block)]
    relax_rate = [relax[:, k, :] for k in range(per_block)]
    for t in range(subs):
        pieces = []
        for s in range(ny):
            value = got_main[s, t * tile : (t + 1) * tile]
            if s:
                moved = pltpu.roll(ghosts[s - 1], lanes - t, 1) if t else ghosts[s - 1]
                value = value + jnp.where(lane % nodes_y == 0, moved, 0.0)
            pieces.append(value)

        def drive(f, k):
            at = (f * per_block + k) * nodes_y
            total = None
            for s in range(ny):
                shift = (s * nodes_y - at) % lanes
                moved = pltpu.roll(pieces[s], shift, 1) if shift else pieces[s]
                total = moved if total is None else jnp.where(lane_y // nodes_y == s, moved, total)
            return total

        for k in range(per_block):
            squared = drive(0, k)
            squared = squared * squared
            binding = squared / (squared + half_square)
            bound[k] = bound[k] + step_size * (
                bind_rate * binding * (1.0 - bound[k]) - unbind_rate[k] * bound[k]
            )
            active[k] = active[k] + step_size * relax_rate[k] * (
                peak_tension * drive(1, k) * bound[k] - active[k]
            )
    for k in range(per_block):
        out_bound[:, k, :] = bound[k]
        out_active[:, k, :] = active[k]

    each_main(lambda copy: copy.wait_send(), chunks, pl.ds(0, third.shape[0]))
    each_edge(lambda copy: copy.wait_send())

    def sent(i, slab_i):
        pltpu.make_async_remote_copy(
            src_ref=got_main.at[pl.ds(ny + i * half, half)],
            dst_ref=got_main.at[pl.ds(0, half)],
            send_sem=send_relay.at[i],
            recv_sem=recv_main.at[gy],
            device_id=(gx, slab_i, column * half),
            device_id_type=MESH,
        ).wait_send()

    far_slabs(sent)


def store_results(bound, active, out_bound, out_active, sem):
    copies = (
        pltpu.make_async_copy(bound, out_bound, sem.at[0]),
        pltpu.make_async_copy(active, out_active, sem.at[1]),
    )
    for copy in copies:
        copy.start()
    for copy in copies:
        copy.wait()


def per_device(calcium, activation, e1, o1, e2, o2, e3, o3, troponin, tension, unbind, relax, *, sizes):
    nx, ny, nz = sizes
    subs, rows, depth, cols = calcium.shape
    nodes_x, per_block, all_y = troponin.shape
    lanes = 2 * per_block * (all_y // ny)
    blocks = nz
    long = (subs + 1) * nodes_x
    short = (subs // per_block + 1) * nodes_x
    vmem = pl.BlockSpec(memory_space=pltpu.VMEM)
    hbm = pl.BlockSpec(memory_space=pltpu.MemorySpace.HBM)
    dma = pltpu.SemaphoreType.DMA
    flat = [x.reshape(1, -1) for x in (e1, o1, e2, o2, e3, o3)]
    shape = jax.ShapeDtypeStruct(troponin.shape, f32)
    operands = [
        pltpu.with_memory_space_constraint(x, pltpu.MemorySpace.HBM)
        for x in (calcium, activation, *flat, troponin, tension, unbind, relax)
    ]
    results = pl.pallas_call(
        functools.partial(kernel, sizes=sizes),
        out_shape=(shape, shape),
        in_specs=[hbm] * 12,
        out_specs=(vmem, vmem),
        scratch_shapes=[
            pltpu.VMEM((2, *calcium.shape), f32),
            *[pltpu.VMEM(x.shape, x.dtype) for x in (*flat, troponin, tension, unbind, relax)],
            pltpu.VMEM((blocks, long, lanes), f32),
            pltpu.VMEM((short, lanes), f32),
            pltpu.VMEM((blocks + 1, subs + 1, lanes), f32),
            pltpu.VMEM((ny + (blocks // 2) ** 2, long, lanes), f32),
            pltpu.VMEM((ny, short, lanes), f32),
            pltpu.VMEM((ny, 2, subs + 1, lanes), f32),
            dma((10 + subs,)),
            dma((blocks // 2,)),
            dma((ny + blocks // 2 * (subs // 2),)),
            dma((ny,)),
            dma((ny,)),
        ],
        compiler_params=pltpu.CompilerParams(
            collective_id=0,
            has_side_effects=True,
            vmem_limit_bytes=32 * 1024 * 1024,
        ),
        name="restrict_steps",
    )(*operands)
    results = [pltpu.with_memory_space_constraint(x, pltpu.MemorySpace.VMEM) for x in results]
    return pl.pallas_call(
        store_results,
        out_shape=(shape, shape),
        in_specs=[vmem] * 2,
        out_specs=(hbm, hbm),
        scratch_shapes=[dma((2,))],
        name="store_results",
    )(*results)


def solution(mesh):
    sizes = tuple(mesh.shape[name] for name in ("gx", "gy", "gz"))
    field = P(None, "gx", "gz", "gy")
    nodes = P("gx", ("gy", "gz"), None)
    return jax.shard_map(
        functools.partial(per_device, sizes=sizes),
        mesh=mesh,
        in_specs=(field, field, P(), P(), P(), P(), P(), P(), nodes, nodes, nodes, nodes),
        out_specs=(nodes, nodes),
        check_vma=False,
    )
```

```python
import functools

import jax
import jax.numpy as jnp
from jax import lax
from jax.experimental import pallas as pl
from jax.experimental.pallas import tpu as pltpu
from jax.sharding import PartitionSpec as P

step_size = 0.2
bind_rate = 2.0
peak_tension = 2.0
half_square = 0.25
f32 = jnp.float32
bf16 = jnp.bfloat16
MESH = pl.DeviceIdType.MESH


def split(x):
    high = x.astype(bf16)
    return high, (x - high.astype(f32)).astype(bf16)


def node_weights(element, offset, node):
    raw = jnp.where(element == node, 1.0 - offset, 0.0) + jnp.where(
        element + 1 == node, offset, 0.0
    )
    total = jnp.sum(raw, axis=1, keepdims=True)
    return raw, jnp.where(total > 0.0, total, 1.0)


def expand(weight, pick):
    high, low = split(weight)
    return jnp.dot(high, pick, preferred_element_type=f32) + jnp.dot(
        low, pick, preferred_element_type=f32
    )


def iota(shape, dim):
    return lax.broadcasted_iota(jnp.int32, shape, dim)


def kernel(
    calcium,
    activation,
    *refs,
    sizes,
):
    small = refs[:10]
    out_bound, out_active, x = refs[10:13]
    local = refs[13:23]
    (
        main,
        third,
        edge,
        got_main,
        got_third,
        got_edge,
        pool,
        send_relay,
        recv_main,
        recv_third,
        recv_edge,
    ) = refs[23:]
    e1, o1, e2, o2, e3, o3, troponin, tension, unbind, relax = local
    nx, ny, nz = sizes
    _, subs, rows, depth, cols = x.shape
    nodes_x, per_block, all_y = troponin.shape
    nodes_y = all_y // ny
    blocks = nz
    slab = per_block * blocks
    gx, gy, gz = lax.axis_index("gx"), lax.axis_index("gy"), lax.axis_index("gz")
    groups = [[t, t + 1] for t in range(0, subs, 2)]
    cuts = [group[-1] + 1 for group in groups]
    chunks = len(cuts)

    def load(t):
        at = len(small) + t
        return [
            pltpu.make_async_copy(field.at[t], x.at[f, t], pool.at[at])
            for f, field in enumerate((calcium, activation))
        ]

    def loaded(t):
        at = len(small) + t
        pltpu.make_async_copy(calcium.at[pl.ds(0, 2)], x.at[:, t], pool.at[at]).wait()

    fetches = [
        pltpu.make_async_copy(source, target, pool.at[i])
        for i, (source, target) in enumerate(zip(small, local))
    ]
    for copy in fetches:
        copy.start()
    for t in range(subs):
        for copy in load(t):
            copy.start(priority=1)

    barrier = pltpu.get_barrier_semaphore()
    has_next_x = gx + 1 < nx
    has_next_z = gz + 1 < nz
    own = gy == gz
    from_third = jnp.logical_and(gz == 0, gy > 0)
    from_first = gx > 0
    from_corner = jnp.logical_and(from_third, from_first)
    half = blocks // 2
    column = gz // half
    home = gy // half
    last = gz % half == half - 1
    crossing = column != home

    def hello(*device):
        pl.semaphore_signal(barrier, inc=1, device_id=device, device_id_type=MESH)

    def far_slabs(do):
        for i in range(half):
            slab_i = (1 - column) * half + i

            @pl.when(jnp.logical_and(last, slab_i != gy))
            def _(i=i, slab_i=slab_i):
                do(i, slab_i)

    far_slabs(lambda i, slab_i: hello(gx, gy, slab_i))
    for s in range(ny):

        def greet(dx, dz, s=s):
            pl.semaphore_signal(
                barrier, inc=1, device_id=(gx - dx, s, gy - dz), device_id_type=MESH
            )

        @pl.when(jnp.logical_not(jnp.logical_and(s == gy, own)))
        def _():
            greet(0, 0)

        @pl.when(jnp.logical_and(crossing, s != gy))
        def _(s=s):
            hello(gx, s, column * half + half - 1)

        @pl.when(jnp.logical_and(from_third, jnp.logical_not(jnp.logical_and(s == gy, gy - 1 == gz))))
        def _():
            greet(0, 1)

        @pl.when(from_first)
        def _():
            greet(1, 0)

        @pl.when(from_corner)
        def _():
            greet(1, 1)

    for copy in fetches[:6]:
        copy.wait()
    tile = nodes_x
    seg = per_block * nodes_y
    lanes = 2 * seg
    first_side = (blocks + 2) * tile
    other_side = (blocks + 1) * tile
    row_count = first_side + (per_block - 1) * other_side
    r = iota((row_count, 1), 0)
    side = jnp.where(r < first_side, 0, (r - first_side) // other_side + 1)
    place = jnp.where(r < first_side, r, (r - first_side) % other_side)
    inner = place < jnp.where(r < first_side, first_side, other_side) - tile
    node_a = jnp.where(inner, place % tile, nodes_x)
    node_b = per_block * jnp.where(inner, place // tile, place % tile) + side
    raw, total = node_weights(e1[...], o1[...], node_a + gx * nodes_x)
    wide = rows * depth
    pick = (
        iota((raw.shape[1], wide), 0) == gx * rows + iota((raw.shape[1], wide), 1) // depth
    ).astype(bf16)
    weight_x = expand(raw / total, pick)
    raw, total = node_weights(e3[...], o3[...], node_b + gz * slab)
    pick = (
        iota((raw.shape[1], wide), 0) == gz * depth + iota((raw.shape[1], wide), 1) % depth
    ).astype(bf16)
    weight_z = expand(raw / total, pick)
    k_high, k_low = split(weight_x * weight_z)
    k_both = jnp.concatenate([k_high, k_low], axis=0)

    def y_weights():
        n = iota((lanes, 1), 0)
        mine = pl.ds(pl.multiple_of(gy * cols, cols), cols)
        spot = n % seg
        beyond = jnp.logical_and(spot >= nodes_y, spot % subs == nodes_y % subs)
        beyond = jnp.logical_and(beyond, spot < nodes_y + per_block * subs)
        node = gy * nodes_y + jnp.where(spot < nodes_y, spot, nodes_y)
        total = node_weights(e2[...], o2[...], node)[1]
        weight = node_weights(e2[:, mine], o2[:, mine], node)[0] / total
        weight = jnp.where(jnp.logical_or(spot < nodes_y, beyond), weight, 0.0).T
        field = iota(weight.shape, 1) // seg
        weight = jnp.concatenate([jnp.where(field == f, weight, 0.0) for f in range(2)], axis=0)
        return jnp.concatenate(split(weight), axis=1)

    def to_message(node, y_both):
        count = node.shape[0]
        out = jnp.dot(
            jnp.concatenate(split(node), axis=0), y_both, preferred_element_type=f32
        )
        return out[:count, :lanes] + out[:count, lanes:] + out[count:, :lanes]

    def span(first, last):
        stop = last * tile + (tile if last == subs else 0)
        return pl.ds(first * tile, stop - first * tile)

    def part(c):
        return span(cuts[c - 1] if c else 0, cuts[c])

    def main_copy(q, c):
        where = part(c) if c < chunks else span(0, subs)
        direct = jnp.int32(1) if c == chunks - 1 else is_direct(q).astype(jnp.int32)
        over = 1 - direct
        line = gz % half
        slot = line * half + q % half
        return pltpu.make_async_remote_copy(
            src_ref=main.at[q, where],
            dst_ref=got_main.at[direct * gy + over * (ny + slot), where],
            send_sem=pool.at[q],
            recv_sem=recv_main.at[direct * gy + over * (ny + line * (chunks - 1) + c % (chunks - 1))],
            device_id=(
                gx,
                direct * gz + over * gy,
                direct * q + over * (q // half * half + half - 1),
            ),
            device_id_type=MESH,
        )

    def forward(i, slab_i, j, c):
        where = part(c) if c < chunks else span(0, subs)
        return pltpu.make_async_remote_copy(
            src_ref=got_main.at[ny + i * half + j, where],
            dst_ref=got_main.at[gy, where],
            send_sem=send_relay.at[i],
            recv_sem=recv_main.at[gy],
            device_id=(gx, slab_i, column * half + j),
            device_id_type=MESH,
        )

    def third_copy():
        return pltpu.make_async_remote_copy(
            src_ref=third,
            dst_ref=got_third.at[gy],
            send_sem=pool.at[blocks],
            recv_sem=recv_third.at[gy],
            device_id=(gx, gz + 1, 0),
            device_id_type=MESH,
        )

    def edge_copy(q, corner):
        return pltpu.make_async_remote_copy(
            src_ref=edge.at[q],
            dst_ref=got_edge.at[gy, corner],
            send_sem=pool.at[len(small) + q],
            recv_sem=recv_edge.at[gy],
            device_id=(gx + 1, gz + corner, 0 if corner else q),
            device_id_type=MESH,
        )

    third_here = jnp.logical_and(gz == 0, gy == 1)
    third_away = jnp.logical_and(has_next_z, jnp.logical_not(third_here))

    holding = jnp.logical_and(last, gy > gz)

    def is_direct(q):
        return jnp.logical_or(own, column == q // half)

    def each_main(do, c, wanted=lambda q: True):
        for q in range(blocks):

            @pl.when(jnp.logical_and(wanted(q), jnp.logical_not(jnp.logical_and(own, gz == q))))
            def _(q=q):
                do(main_copy(q, c))

    def held(q):
        return holding

    def send(c):
        final = c == chunks - 1
        wanted = (lambda q: jnp.logical_not(held(q))) if final else (lambda q: True)
        each_main(lambda copy: copy.start(), c, wanted)

    def send_rest():
        @pl.when(third_away)
        def _():
            third_copy().start()

        each_edge(lambda copy: copy.start())

    late = jnp.logical_or(gy < gz, gy == 0)

    def meet():
        extra = blocks + has_next_z.astype(jnp.int32)
        count = jnp.where(has_next_x, extra, 0)
        count = count + jnp.where(own, blocks - 1, blocks + 1)
        count = count + third_away.astype(jnp.int32)
        served = half - crossing.astype(jnp.int32)
        count = count + jnp.where(last, served * half, 0)
        pl.semaphore_wait(barrier, count)

    def each_edge(do):
        @pl.when(has_next_x)
        def _():
            for q in range(blocks):
                do(edge_copy(q, 0))

        @pl.when(jnp.logical_and(has_next_x, has_next_z))
        def _():
            do(edge_copy(blocks, 1))

    spot = iota((tile, lanes), 1) % seg
    pieces = blocks + 2
    state = {"packed": None, "pair": None}

    def nodes_of(group):
        nodes = []
        for t in group:
            high, low = split(
                jnp.concatenate([x[f, t].reshape(wide, cols) for f in range(2)], axis=1)
            )
            both = jnp.dot(k_both, high, preferred_element_type=f32)
            nodes.append(
                both[:row_count]
                + both[row_count:]
                + jnp.dot(k_high, low, preferred_element_type=f32)
            )
        return jnp.concatenate(nodes, axis=0)

    def place_message(t, values):
        main_tiles, ghost_tiles = [], []
        for i in range(pieces):
            total, ghost = values[i * tile : (i + 1) * tile], 0.0
            here = total
            for k in range(per_block):
                if k and i == blocks:
                    here = None
                elif k:
                    at = first_side + (k - 1) * other_side + (i - (i > blocks)) * tile
                    here = values[at : at + tile]
                in_place = spot // nodes_y == k
                if k:
                    total = jnp.where(in_place, 0.0 if here is None else pltpu.roll(here, k * nodes_y, 1), total)
                if here is not None:
                    ghost = jnp.where(spot == nodes_y + k * subs, here, ghost)
            main_tiles.append(total)
            ghost_tiles.append(pltpu.roll(ghost, t, 1) if t else ghost)
        for q in range(blocks):
            main[q, t * tile : (t + 1) * tile] = main_tiles[q]
        for q in range(blocks + 1):
            edge[q, t : t + 1] = main_tiles[blocks + 1][q : q + 1]
        above = main_tiles[blocks]
        fold = t % per_block
        state["pair"] = pltpu.roll(above, fold * nodes_y, 1) + state["pair"] if fold else above
        if fold == per_block - 1:
            at = t // per_block * tile
            third[at : at + tile] = state["pair"]
        packed = state["packed"]
        packed = ghost_tiles if packed is None else [x + y for x, y in zip(packed, ghost_tiles)]
        state["packed"] = packed
        if t == subs - 1:
            for q in range(blocks):
                main[q, subs * tile : (subs + 1) * tile] = packed[q]
            at = subs // per_block * tile
            third[at : at + tile] = packed[blocks]
            for q in range(blocks + 1):
                edge[q, subs : subs + 1] = packed[blocks + 1][q : q + 1]

    y_both = node = None
    for g in range(len(groups) + 1):
        group = groups[g] if g < len(groups) else []
        for t in group:
            loaded(t)
        before, node = node, nodes_of(group) if group else None
        if g == 0:
            y_both = y_weights()
            continue
        values = to_message(before, y_both)
        for i, t in enumerate(groups[g - 1]):
            place_message(t, values[i * row_count : (i + 1) * row_count])
        c = g - 1
        if c < chunks - 2:

            @pl.when(jnp.logical_not(late))
            def _(c=c):
                if c == 0:
                    meet()
                send(c)

            continue
        if c == chunks - 2:

            @pl.when(late)
            def _(c=c):
                meet()
                for before_c in range(c):
                    send(before_c)

        send(c)

    @pl.when(jnp.logical_not(holding))
    def _():
        send_rest()

    for copy in fetches[6:]:
        copy.wait()

    for c in range(chunks - 1):

        def pass_on(i, slab_i, c=c):
            pltpu.make_async_remote_copy(
                src_ref=main.at[pl.ds(0, half), part(c)],
                dst_ref=got_main.at[pl.ds(ny + i * half, half), part(c)],
                send_sem=pool.at[0],
                recv_sem=recv_main.at[ny + i * (chunks - 1) + c],
                device_id=(gx, gy, gz),
                device_id_type=MESH,
            ).wait_recv()
            for j in range(half):
                forward(i, slab_i, j, c).start()

        if c == chunks - 2:

            @pl.when(holding)
            def _():
                each_main(lambda copy: copy.start(), chunks - 1, held)
                send_rest()

        far_slabs(pass_on)

    @pl.when(own)
    def _():
        got_main[gy] = main[gz]

    @pl.when(third_here)
    def _():
        got_third[gy] = third[...]

    for s in range(ny):

        @pl.when(jnp.logical_not(jnp.logical_and(own, gy == s)))
        def _(s=s):
            pltpu.make_async_remote_copy(
                src_ref=main.at[0],
                dst_ref=got_main.at[s],
                send_sem=pool.at[0],
                recv_sem=recv_main.at[s],
                device_id=(gx, gy, gz),
                device_id_type=MESH,
            ).wait_recv()

    @pl.when(from_third)
    def _():
        for s in range(ny):

            @pl.when(jnp.logical_not(jnp.logical_and(gy == 1, jnp.logical_and(gz == 0, s == gy)) & (gz == gy - 1)))
            def _(s=s):
                pltpu.make_async_remote_copy(
                    src_ref=third,
                    dst_ref=got_third.at[s],
                    send_sem=pool.at[0],
                    recv_sem=recv_third.at[s],
                    device_id=(gx, gy, gz),
                    device_id_type=MESH,
                ).wait_recv()

            first_block = iota((tile, lanes), 1) // nodes_y % per_block == 0
            for t in range(subs):
                at = t // per_block * tile
                moved = got_third[s, at : at + tile]
                place = t % per_block
                if place:
                    moved = pltpu.roll(moved, lanes - place * nodes_y, 1)
                rows_t = pl.ds(t * tile, tile)
                got_main[s, rows_t] = got_main[s, rows_t] + jnp.where(first_block, moved, 0.0)
            at = subs // per_block * tile
            rows_t = pl.ds(subs * tile, tile)
            got_main[s, rows_t] = got_main[s, rows_t] + got_third[s, at : at + tile]

    def add_edge(corners):
        for s in range(ny):
            pltpu.make_async_remote_copy(
                src_ref=edge.at[pl.ds(0, 1 + corners)],
                dst_ref=got_edge.at[s, pl.ds(0, 1 + corners)],
                send_sem=pool.at[0],
                recv_sem=recv_edge.at[s],
                device_id=(gx, gy, gz),
                device_id_type=MESH,
            ).wait_recv()
            for t in range(subs + 1):
                at = pl.ds(t * tile, 1)
                total = got_main[s, at]
                for corner in range(1 + corners):
                    total = total + got_edge[s, corner, t : t + 1]
                got_main[s, at] = total

    @pl.when(jnp.logical_and(from_first, jnp.logical_not(from_corner)))
    def _():
        add_edge(0)

    @pl.when(from_corner)
    def _():
        add_edge(1)

    lane = iota((tile, lanes), 1)
    lane_y = iota((tile, all_y), 1)
    ghosts = []
    for s in range(ny - 1):
        raw = got_main[s, subs * tile : (subs + 1) * tile]
        ghost = pltpu.roll(raw, lanes - nodes_y, 1)
        for k in range(1, per_block):
            moved = pltpu.roll(raw, (lanes + k * nodes_y - nodes_y - k * subs) % lanes, 1)
            ghost = jnp.where(spot // nodes_y == k, moved, ghost)
        ghosts.append(ghost)
    bound = [troponin[:, k, :] for k in range(per_block)]
    active = [tension[:, k, :] for k in range(per_block)]
    unbind_rate = [unbind[:, k, :] for k in range(per_block)]
    relax_rate = [relax[:, k, :] for k in range(per_block)]
    for t in range(subs):
        pieces = []
        for s in range(ny):
            value = got_main[s, t * tile : (t + 1) * tile]
            if s:
                moved = pltpu.roll(ghosts[s - 1], lanes - t, 1) if t else ghosts[s - 1]
                value = value + jnp.where(lane % nodes_y == 0, moved, 0.0)
            pieces.append(value)

        def drive(f, k):
            at = (f * per_block + k) * nodes_y
            total = None
            for s in range(ny):
                shift = (s * nodes_y - at) % lanes
                moved = pltpu.roll(pieces[s], shift, 1) if shift else pieces[s]
                total = moved if total is None else jnp.where(lane_y // nodes_y == s, moved, total)
            return total

        for k in range(per_block):
            squared = drive(0, k)
            squared = squared * squared
            binding = squared / (squared + half_square)
            bound[k] = bound[k] + step_size * (
                bind_rate * binding * (1.0 - bound[k]) - unbind_rate[k] * bound[k]
            )
            active[k] = active[k] + step_size * relax_rate[k] * (
                peak_tension * drive(1, k) * bound[k] - active[k]
            )
    for k in range(per_block):
        out_bound[:, k, :] = bound[k]
        out_active[:, k, :] = active[k]

    each_main(lambda copy: copy.wait_send(), chunks)

    @pl.when(third_away)
    def _():
        third_copy().wait_send()

    each_edge(lambda copy: copy.wait_send())

    def sent(i, slab_i):
        pltpu.make_async_remote_copy(
            src_ref=got_main.at[pl.ds(ny + i * half, half), span(0, cuts[-2])],
            dst_ref=got_main.at[pl.ds(0, half), span(0, cuts[-2])],
            send_sem=send_relay.at[i],
            recv_sem=recv_main.at[gy],
            device_id=(gx, slab_i, column * half),
            device_id_type=MESH,
        ).wait_send()

    far_slabs(sent)


def store_results(bound, active, out_bound, out_active, sem):
    copies = (
        pltpu.make_async_copy(bound, out_bound, sem.at[0]),
        pltpu.make_async_copy(active, out_active, sem.at[1]),
    )
    for copy in copies:
        copy.start()
    for copy in copies:
        copy.wait()


def per_device(calcium, activation, e1, o1, e2, o2, e3, o3, troponin, tension, unbind, relax, *, sizes):
    nx, ny, nz = sizes
    subs, rows, depth, cols = calcium.shape
    nodes_x, per_block, all_y = troponin.shape
    lanes = 2 * per_block * (all_y // ny)
    blocks = nz
    long = (subs + 1) * nodes_x
    short = (subs // per_block + 1) * nodes_x
    vmem = pl.BlockSpec(memory_space=pltpu.VMEM)
    hbm = pl.BlockSpec(memory_space=pltpu.MemorySpace.HBM)
    dma = pltpu.SemaphoreType.DMA
    flat = [x.reshape(1, -1) for x in (e1, o1, e2, o2, e3, o3)]
    shape = jax.ShapeDtypeStruct(troponin.shape, f32)
    operands = [
        pltpu.with_memory_space_constraint(x, pltpu.MemorySpace.HBM)
        for x in (calcium, activation, *flat, troponin, tension, unbind, relax)
    ]
    results = pl.pallas_call(
        functools.partial(kernel, sizes=sizes),
        out_shape=(shape, shape),
        in_specs=[hbm] * 12,
        out_specs=(vmem, vmem),
        scratch_shapes=[
            pltpu.VMEM((2, *calcium.shape), f32),
            *[pltpu.VMEM(x.shape, x.dtype) for x in (*flat, troponin, tension, unbind, relax)],
            pltpu.VMEM((blocks, long, lanes), f32),
            pltpu.VMEM((short, lanes), f32),
            pltpu.VMEM((blocks + 1, subs + 1, lanes), f32),
            pltpu.VMEM((ny + (blocks // 2) ** 2, long, lanes), f32),
            pltpu.VMEM((ny, short, lanes), f32),
            pltpu.VMEM((ny, 2, subs + 1, lanes), f32),
            dma((10 + subs,)),
            dma((blocks // 2,)),
            dma((ny + blocks // 2 * (subs // 2 - 1),)),
            dma((ny,)),
            dma((ny,)),
        ],
        compiler_params=pltpu.CompilerParams(
            collective_id=0,
            has_side_effects=True,
            vmem_limit_bytes=32 * 1024 * 1024,
        ),
        name="restrict_steps",
    )(*operands)
    results = [pltpu.with_memory_space_constraint(x, pltpu.MemorySpace.VMEM) for x in results]
    return pl.pallas_call(
        store_results,
        out_shape=(shape, shape),
        in_specs=[vmem] * 2,
        out_specs=(hbm, hbm),
        scratch_shapes=[dma((2,))],
        name="store_results",
    )(*results)


def solution(mesh):
    sizes = tuple(mesh.shape[name] for name in ("gx", "gy", "gz"))
    field = P(None, "gx", "gz", "gy")
    nodes = P("gx", ("gy", "gz"), None)
    return jax.shard_map(
        functools.partial(per_device, sizes=sizes),
        mesh=mesh,
        in_specs=(field, field, P(), P(), P(), P(), P(), P(), nodes, nodes, nodes, nodes),
        out_specs=(nodes, nodes),
        check_vma=False,
    )
```

```python
import functools

import jax
import jax.numpy as jnp
from jax import lax
from jax.experimental import pallas as pl
from jax.experimental.pallas import tpu as pltpu
from jax.sharding import PartitionSpec as P

step_size = 0.2
bind_rate = 2.0
peak_tension = 2.0
half_square = 0.25
f32 = jnp.float32
bf16 = jnp.bfloat16
MESH = pl.DeviceIdType.MESH


def split(x):
    high = x.astype(bf16)
    return high, (x - high.astype(f32)).astype(bf16)


def node_weights(element, offset, node):
    raw = jnp.where(element == node, 1.0 - offset, 0.0) + jnp.where(
        element + 1 == node, offset, 0.0
    )
    total = jnp.sum(raw, axis=1, keepdims=True)
    return raw, jnp.where(total > 0.0, total, 1.0)


def expand(weight, pick):
    high, low = split(weight)
    return jnp.dot(high, pick, preferred_element_type=f32) + jnp.dot(
        low, pick, preferred_element_type=f32
    )


def iota(shape, dim):
    return lax.broadcasted_iota(jnp.int32, shape, dim)


def kernel(
    calcium,
    activation,
    *refs,
    sizes,
):
    small = refs[:10]
    out_bound, out_active, x = refs[10:13]
    local = refs[13:23]
    (
        main,
        third,
        edge,
        got_main,
        got_third,
        got_edge,
        pool,
        recv_main,
        recv_third,
        recv_edge,
    ) = refs[23:]
    e1, o1, e2, o2, e3, o3, troponin, tension, unbind, relax = local
    nx, ny, nz = sizes
    subs = calcium.shape[0]
    rows, depth, cols = x.shape[2:]
    nodes_x, per_block, all_y = troponin.shape
    nodes_y = all_y // ny
    blocks = nz
    slab = per_block * blocks
    gx, gy, gz = lax.axis_index("gx"), lax.axis_index("gy"), lax.axis_index("gz")
    groups = [[t, t + 1] for t in range(0, subs, 2)]
    cuts = [group[-1] + 1 for group in groups]
    chunks = len(cuts)

    def load(g):
        return [
            pltpu.make_async_copy(
                field.at[pl.ds(2 * g, 2)], x.at[g, pl.ds(2 * f, 2)], pool.at[len(small) + g]
            )
            for f, field in enumerate((calcium, activation))
        ]

    def loaded(g):
        pltpu.make_async_copy(calcium.at[pl.ds(0, 4)], x.at[g], pool.at[len(small) + g]).wait()

    fetches = [
        pltpu.make_async_copy(source, target, pool.at[i])
        for i, (source, target) in enumerate(zip(small, local))
    ]
    for copy in fetches:
        copy.start()
    for g in range(subs // 2):
        for copy in load(g):
            copy.start(priority=1)

    barrier = pltpu.get_barrier_semaphore()
    has_next_x = gx + 1 < nx
    has_next_z = gz + 1 < nz
    own = gy == gz
    from_third = jnp.logical_and(gz == 0, gy > 0)
    from_first = gx > 0
    from_corner = jnp.logical_and(from_third, from_first)
    half = blocks // 2
    column = gz // half
    home = gy // half
    last = gz % half == half - 1
    crossing = column != home

    def hello(*device):
        pl.semaphore_signal(barrier, inc=1, device_id=device, device_id_type=MESH)

    def far_slabs(do):
        for i in range(half):
            slab_i = (1 - column) * half + i

            @pl.when(jnp.logical_and(last, slab_i != gy))
            def _(i=i, slab_i=slab_i):
                do(i, slab_i)

    far_slabs(lambda i, slab_i: hello(gx, gy, slab_i))
    for s in range(ny):

        def greet(dx, dz, s=s):
            pl.semaphore_signal(
                barrier, inc=1, device_id=(gx - dx, s, gy - dz), device_id_type=MESH
            )

        @pl.when(jnp.logical_not(jnp.logical_and(s == gy, own)))
        def _():
            greet(0, 0)

        @pl.when(jnp.logical_and(crossing, s != gy))
        def _(s=s):
            hello(gx, s, column * half + half - 1)

        @pl.when(jnp.logical_and(from_third, jnp.logical_not(jnp.logical_and(s == gy, gy - 1 == gz))))
        def _():
            greet(0, 1)

        @pl.when(from_first)
        def _():
            greet(1, 0)

        @pl.when(from_corner)
        def _():
            greet(1, 1)

    for copy in fetches[:6]:
        copy.wait()
    tile = nodes_x
    seg = per_block * nodes_y
    lanes = 2 * seg
    first_side = (blocks + 2) * tile
    other_side = (blocks + 1) * tile
    row_count = first_side + (per_block - 1) * other_side
    r = iota((row_count, 1), 0)
    side = jnp.where(r < first_side, 0, (r - first_side) // other_side + 1)
    place = jnp.where(r < first_side, r, (r - first_side) % other_side)
    inner = place < jnp.where(r < first_side, first_side, other_side) - tile
    node_a = jnp.where(inner, place % tile, nodes_x)
    node_b = per_block * jnp.where(inner, place // tile, place % tile) + side
    raw, total = node_weights(e1[...], o1[...], node_a + gx * nodes_x)
    wide = rows * depth
    pick = (
        iota((raw.shape[1], wide), 0) == gx * rows + iota((raw.shape[1], wide), 1) // depth
    ).astype(bf16)
    weight_x = expand(raw / total, pick)
    raw, total = node_weights(e3[...], o3[...], node_b + gz * slab)
    pick = (
        iota((raw.shape[1], wide), 0) == gz * depth + iota((raw.shape[1], wide), 1) % depth
    ).astype(bf16)
    weight_z = expand(raw / total, pick)
    k_high, k_low = split(weight_x * weight_z)
    k_both = jnp.concatenate([k_high, k_low], axis=0)

    def y_weights():
        n = iota((lanes, 1), 0)
        mine = pl.ds(pl.multiple_of(gy * cols, cols), cols)
        spot = n % seg
        beyond = jnp.logical_and(spot >= nodes_y, spot % subs == nodes_y % subs)
        beyond = jnp.logical_and(beyond, spot < nodes_y + per_block * subs)
        node = gy * nodes_y + jnp.where(spot < nodes_y, spot, nodes_y)
        total = node_weights(e2[...], o2[...], node)[1]
        weight = node_weights(e2[:, mine], o2[:, mine], node)[0] / total
        weight = jnp.where(jnp.logical_or(spot < nodes_y, beyond), weight, 0.0).T
        field = iota(weight.shape, 1) // seg
        weight = jnp.concatenate([jnp.where(field == f, weight, 0.0) for f in range(2)], axis=0)
        return jnp.concatenate(split(weight), axis=1)

    def to_message(node, y_both):
        count = node.shape[0]
        out = jnp.dot(
            jnp.concatenate(split(node), axis=0), y_both, preferred_element_type=f32
        )
        return out[:count, :lanes] + out[:count, lanes:] + out[count:, :lanes]

    def span(first, last):
        stop = last * tile + (tile if last == subs else 0)
        return pl.ds(first * tile, stop - first * tile)

    def part(c):
        return span(cuts[c - 1] if c else 0, cuts[c])

    def main_copy(q, c):
        where = part(c) if c < chunks else span(0, subs)
        direct = jnp.int32(1) if c == chunks - 1 else is_direct(q).astype(jnp.int32)
        over = 1 - direct
        line = gz % half
        slot = line * half + q % half
        return pltpu.make_async_remote_copy(
            src_ref=main.at[q, where],
            dst_ref=got_main.at[direct * gy + over * (ny + slot), where],
            send_sem=pool.at[q],
            recv_sem=recv_main.at[direct * gy + over * (ny + line * (chunks - 1) + c % (chunks - 1))],
            device_id=(
                gx,
                direct * gz + over * gy,
                direct * q + over * (q // half * half + half - 1),
            ),
            device_id_type=MESH,
        )

    def forward(i, slab_i, j, c):
        where = part(c) if c < chunks else span(0, subs)
        return pltpu.make_async_remote_copy(
            src_ref=got_main.at[ny + i * half + j, where],
            dst_ref=got_main.at[gy, where],
            send_sem=pool.at[6 + i],
            recv_sem=recv_main.at[gy],
            device_id=(gx, slab_i, column * half + j),
            device_id_type=MESH,
        )

    def third_copy():
        return pltpu.make_async_remote_copy(
            src_ref=third,
            dst_ref=got_third.at[gy],
            send_sem=pool.at[blocks],
            recv_sem=recv_third.at[gy],
            device_id=(gx, gz + 1, 0),
            device_id_type=MESH,
        )

    def edge_copy(q, corner):
        return pltpu.make_async_remote_copy(
            src_ref=edge.at[q],
            dst_ref=got_edge.at[gy, corner],
            send_sem=pool.at[len(small) - 5 if corner else len(small) + q],
            recv_sem=recv_edge.at[gy],
            device_id=(gx + 1, gz + corner, 0 if corner else q),
            device_id_type=MESH,
        )

    third_here = jnp.logical_and(gz == 0, gy == 1)
    third_away = jnp.logical_and(has_next_z, jnp.logical_not(third_here))

    holding = jnp.logical_and(last, gy > gz)

    def is_direct(q):
        return jnp.logical_or(own, column == q // half)

    def each_main(do, c, wanted=lambda q: True):
        for q in range(blocks):

            @pl.when(jnp.logical_and(wanted(q), jnp.logical_not(jnp.logical_and(own, gz == q))))
            def _(q=q):
                do(main_copy(q, c))

    def held(q):
        return holding

    def send(c):
        final = c == chunks - 1
        wanted = (lambda q: jnp.logical_not(held(q))) if final else (lambda q: True)
        each_main(lambda copy: copy.start(), c, wanted)

    def send_rest():
        @pl.when(third_away)
        def _():
            third_copy().start()

        each_edge(lambda copy: copy.start())

    late = jnp.logical_or(gy < gz, gy == 0)

    def meet():
        extra = blocks + has_next_z.astype(jnp.int32)
        count = jnp.where(has_next_x, extra, 0)
        count = count + jnp.where(own, blocks - 1, blocks + 1)
        count = count + third_away.astype(jnp.int32)
        served = half - crossing.astype(jnp.int32)
        count = count + jnp.where(last, served * half, 0)
        pl.semaphore_wait(barrier, count)

    def each_edge(do):
        @pl.when(has_next_x)
        def _():
            for q in range(blocks):
                do(edge_copy(q, 0))

        @pl.when(jnp.logical_and(has_next_x, has_next_z))
        def _():
            do(edge_copy(blocks, 1))

    spot = iota((tile, lanes), 1) % seg
    pieces = blocks + 2
    state = {"packed": None, "pair": None}

    def nodes_of(group):
        nodes = []
        for t in group:
            high, low = split(
                jnp.concatenate([x[t // 2, 2 * f + t % 2].reshape(wide, cols) for f in range(2)], axis=1)
            )
            both = jnp.dot(k_both, high, preferred_element_type=f32)
            nodes.append(
                both[:row_count]
                + both[row_count:]
                + jnp.dot(k_high, low, preferred_element_type=f32)
            )
        return jnp.concatenate(nodes, axis=0)

    def place_message(t, values):
        main_tiles, ghost_tiles = [], []
        for i in range(pieces):
            total, ghost = values[i * tile : (i + 1) * tile], 0.0
            here = total
            for k in range(per_block):
                if k and i == blocks:
                    here = None
                elif k:
                    at = first_side + (k - 1) * other_side + (i - (i > blocks)) * tile
                    here = values[at : at + tile]
                in_place = spot // nodes_y == k
                if k:
                    total = jnp.where(in_place, 0.0 if here is None else pltpu.roll(here, k * nodes_y, 1), total)
                if here is not None:
                    ghost = jnp.where(spot == nodes_y + k * subs, here, ghost)
            main_tiles.append(total)
            ghost_tiles.append(pltpu.roll(ghost, t, 1) if t else ghost)
        for q in range(blocks):
            main[q, t * tile : (t + 1) * tile] = main_tiles[q]
        for q in range(blocks + 1):
            edge[q, t : t + 1] = main_tiles[blocks + 1][q : q + 1]
        above = main_tiles[blocks]
        fold = t % per_block
        state["pair"] = pltpu.roll(above, fold * nodes_y, 1) + state["pair"] if fold else above
        if fold == per_block - 1:
            at = t // per_block * tile
            third[at : at + tile] = state["pair"]
        packed = state["packed"]
        packed = ghost_tiles if packed is None else [x + y for x, y in zip(packed, ghost_tiles)]
        state["packed"] = packed
        if t == subs - 1:
            for q in range(blocks):
                main[q, subs * tile : (subs + 1) * tile] = packed[q]
            at = subs // per_block * tile
            third[at : at + tile] = packed[blocks]
            for q in range(blocks + 1):
                edge[q, subs : subs + 1] = packed[blocks + 1][q : q + 1]

    y_both = node = None
    for g in range(len(groups) + 1):
        group = groups[g] if g < len(groups) else []
        if group:
            loaded(g)
        before, node = node, nodes_of(group) if group else None
        if g == 0:
            y_both = y_weights()
            continue
        values = to_message(before, y_both)
        for i, t in enumerate(groups[g - 1]):
            place_message(t, values[i * row_count : (i + 1) * row_count])
        c = g - 1
        if c < chunks - 2:

            @pl.when(jnp.logical_not(late))
            def _(c=c):
                if c == 0:
                    meet()
                send(c)

            continue
        if c == chunks - 2:

            @pl.when(late)
            def _(c=c):
                meet()
                for before_c in range(c):
                    send(before_c)

        send(c)

    @pl.when(jnp.logical_not(holding))
    def _():
        send_rest()

    for copy in fetches[6:]:
        copy.wait()

    for c in range(chunks - 1):

        def pass_on(i, slab_i, c=c):
            pltpu.make_async_remote_copy(
                src_ref=main.at[pl.ds(0, half), part(c)],
                dst_ref=got_main.at[pl.ds(ny + i * half, half), part(c)],
                send_sem=pool.at[0],
                recv_sem=recv_main.at[ny + i * (chunks - 1) + c],
                device_id=(gx, gy, gz),
                device_id_type=MESH,
            ).wait_recv()
            for j in range(half):
                forward(i, slab_i, j, c).start()

        if c == chunks - 2:

            @pl.when(holding)
            def _():
                each_main(lambda copy: copy.start(), chunks - 1, held)
                send_rest()

        far_slabs(pass_on)

    @pl.when(own)
    def _():
        got_main[gy] = main[gz]

    @pl.when(third_here)
    def _():
        got_third[gy] = third[...]

    for s in range(ny):

        @pl.when(jnp.logical_not(jnp.logical_and(own, gy == s)))
        def _(s=s):
            pltpu.make_async_remote_copy(
                src_ref=main.at[0],
                dst_ref=got_main.at[s],
                send_sem=pool.at[0],
                recv_sem=recv_main.at[s],
                device_id=(gx, gy, gz),
                device_id_type=MESH,
            ).wait_recv()

    @pl.when(from_third)
    def _():
        for s in range(ny):

            @pl.when(jnp.logical_not(jnp.logical_and(gy == 1, jnp.logical_and(gz == 0, s == gy)) & (gz == gy - 1)))
            def _(s=s):
                pltpu.make_async_remote_copy(
                    src_ref=third,
                    dst_ref=got_third.at[s],
                    send_sem=pool.at[0],
                    recv_sem=recv_third.at[s],
                    device_id=(gx, gy, gz),
                    device_id_type=MESH,
                ).wait_recv()

            first_block = iota((tile, lanes), 1) // nodes_y % per_block == 0
            for t in range(subs):
                at = t // per_block * tile
                moved = got_third[s, at : at + tile]
                place = t % per_block
                if place:
                    moved = pltpu.roll(moved, lanes - place * nodes_y, 1)
                rows_t = pl.ds(t * tile, tile)
                got_main[s, rows_t] = got_main[s, rows_t] + jnp.where(first_block, moved, 0.0)
            at = subs // per_block * tile
            rows_t = pl.ds(subs * tile, tile)
            got_main[s, rows_t] = got_main[s, rows_t] + got_third[s, at : at + tile]

    def add_edge(corners):
        for s in range(ny):
            pltpu.make_async_remote_copy(
                src_ref=edge.at[pl.ds(0, 1 + corners)],
                dst_ref=got_edge.at[s, pl.ds(0, 1 + corners)],
                send_sem=pool.at[0],
                recv_sem=recv_edge.at[s],
                device_id=(gx, gy, gz),
                device_id_type=MESH,
            ).wait_recv()
            for t in range(subs + 1):
                at = pl.ds(t * tile, 1)
                total = got_main[s, at]
                for corner in range(1 + corners):
                    total = total + got_edge[s, corner, t : t + 1]
                got_main[s, at] = total

    @pl.when(jnp.logical_and(from_first, jnp.logical_not(from_corner)))
    def _():
        add_edge(0)

    @pl.when(from_corner)
    def _():
        add_edge(1)

    lane = iota((tile, lanes), 1)
    lane_y = iota((tile, all_y), 1)
    ghosts = []
    for s in range(ny - 1):
        raw = got_main[s, subs * tile : (subs + 1) * tile]
        ghost = pltpu.roll(raw, lanes - nodes_y, 1)
        for k in range(1, per_block):
            moved = pltpu.roll(raw, (lanes + k * nodes_y - nodes_y - k * subs) % lanes, 1)
            ghost = jnp.where(spot // nodes_y == k, moved, ghost)
        ghosts.append(ghost)
    bound = [troponin[:, k, :] for k in range(per_block)]
    active = [tension[:, k, :] for k in range(per_block)]
    unbind_rate = [unbind[:, k, :] for k in range(per_block)]
    relax_rate = [relax[:, k, :] for k in range(per_block)]
    for t in range(subs):
        pieces = []
        for s in range(ny):
            value = got_main[s, t * tile : (t + 1) * tile]
            if s:
                moved = pltpu.roll(ghosts[s - 1], lanes - t, 1) if t else ghosts[s - 1]
                value = value + jnp.where(lane % nodes_y == 0, moved, 0.0)
            pieces.append(value)

        def drive(f, k):
            at = (f * per_block + k) * nodes_y
            total = None
            for s in range(ny):
                shift = (s * nodes_y - at) % lanes
                moved = pltpu.roll(pieces[s], shift, 1) if shift else pieces[s]
                total = moved if total is None else jnp.where(lane_y // nodes_y == s, moved, total)
            return total

        for k in range(per_block):
            squared = drive(0, k)
            squared = squared * squared
            binding = squared / (squared + half_square)
            bound[k] = bound[k] + step_size * (
                bind_rate * binding * (1.0 - bound[k]) - unbind_rate[k] * bound[k]
            )
            active[k] = active[k] + step_size * relax_rate[k] * (
                peak_tension * drive(1, k) * bound[k] - active[k]
            )
    for k in range(per_block):
        out_bound[:, k, :] = bound[k]
        out_active[:, k, :] = active[k]

    each_main(lambda copy: copy.wait_send(), chunks)

    @pl.when(third_away)
    def _():
        third_copy().wait_send()

    each_edge(lambda copy: copy.wait_send())

    def sent(i, slab_i):
        pltpu.make_async_remote_copy(
            src_ref=got_main.at[pl.ds(ny + i * half, half), span(0, cuts[-2])],
            dst_ref=got_main.at[pl.ds(0, half), span(0, cuts[-2])],
            send_sem=pool.at[6 + i],
            recv_sem=recv_main.at[gy],
            device_id=(gx, slab_i, column * half),
            device_id_type=MESH,
        ).wait_send()

    far_slabs(sent)


def store_results(bound, active, out_bound, out_active, sem):
    copies = (
        pltpu.make_async_copy(bound, out_bound, sem.at[0]),
        pltpu.make_async_copy(active, out_active, sem.at[1]),
    )
    for copy in copies:
        copy.start()
    for copy in copies:
        copy.wait()


def per_device(calcium, activation, e1, o1, e2, o2, e3, o3, troponin, tension, unbind, relax, *, sizes):
    nx, ny, nz = sizes
    subs, rows, depth, cols = calcium.shape
    nodes_x, per_block, all_y = troponin.shape
    lanes = 2 * per_block * (all_y // ny)
    blocks = nz
    long = (subs + 1) * nodes_x
    short = (subs // per_block + 1) * nodes_x
    vmem = pl.BlockSpec(memory_space=pltpu.VMEM)
    hbm = pl.BlockSpec(memory_space=pltpu.MemorySpace.HBM)
    dma = pltpu.SemaphoreType.DMA
    flat = [x.reshape(1, -1) for x in (e1, o1, e2, o2, e3, o3)]
    shape = jax.ShapeDtypeStruct(troponin.shape, f32)
    operands = [
        pltpu.with_memory_space_constraint(x, pltpu.MemorySpace.HBM)
        for x in (calcium, activation, *flat, troponin, tension, unbind, relax)
    ]
    results = pl.pallas_call(
        functools.partial(kernel, sizes=sizes),
        out_shape=(shape, shape),
        in_specs=[hbm] * 12,
        out_specs=(vmem, vmem),
        scratch_shapes=[
            pltpu.VMEM((subs // 2, 4, *calcium.shape[1:]), f32),
            *[pltpu.VMEM(x.shape, x.dtype) for x in (*flat, troponin, tension, unbind, relax)],
            pltpu.VMEM((blocks, long, lanes), f32),
            pltpu.VMEM((short, lanes), f32),
            pltpu.VMEM((blocks + 1, subs + 1, lanes), f32),
            pltpu.VMEM((ny + (blocks // 2) ** 2, long, lanes), f32),
            pltpu.VMEM((ny, short, lanes), f32),
            pltpu.VMEM((ny, 2, subs + 1, lanes), f32),
            dma((10 + subs // 2,)),
            dma((ny + blocks // 2 * (subs // 2 - 1),)),
            dma((ny,)),
            dma((ny,)),
        ],
        compiler_params=pltpu.CompilerParams(
            collective_id=0,
            has_side_effects=True,
            vmem_limit_bytes=32 * 1024 * 1024,
        ),
        name="restrict_steps",
    )(*operands)
    results = [pltpu.with_memory_space_constraint(x, pltpu.MemorySpace.VMEM) for x in results]
    return pl.pallas_call(
        store_results,
        out_shape=(shape, shape),
        in_specs=[vmem] * 2,
        out_specs=(hbm, hbm),
        scratch_shapes=[dma((2,))],
        name="store_results",
    )(*results)


def solution(mesh):
    sizes = tuple(mesh.shape[name] for name in ("gx", "gy", "gz"))
    field = P(None, "gx", "gz", "gy")
    nodes = P("gx", ("gy", "gz"), None)
    return jax.shard_map(
        functools.partial(per_device, sizes=sizes),
        mesh=mesh,
        in_specs=(field, field, P(), P(), P(), P(), P(), P(), nodes, nodes, nodes, nodes),
        out_specs=(nodes, nodes),
        check_vma=False,
    )
```
